8 devices in a mesh: data: 2 (over z, y), seq: 4 (over x, core).
Axes of the slice: x: 2, y: 2, z: 1, core: 2. Of those that a mesh axis runs over, the one named last changes fastest.
Arguments:
- x: bfloat16 [4, 1024, 1024], P('data', 'seq'), parts along dimension 0
- w_in: bfloat16 [1024, 3352], replicated
- dt_bias: float32 [24], replicated
- a_neg: float32 [24], replicated
- d_skip: float32 [24], replicated
- w_out: bfloat16 [1536, 1024], replicated
- w_up1: bfloat16 [1024, 4096], replicated
- w_down1: bfloat16 [2048, 1024], replicated
- w_q: bfloat16 [1024, 8, 64], replicated
- w_kv: bfloat16 [1024, 2, 2, 64], replicated
- w_o: bfloat16 [8, 64, 1024], replicated
- w_up2: bfloat16 [1024, 4096], replicated
- w_down2: bfloat16 [2048, 1024], replicated
Outputs:
- output: bfloat16 [4, 1024, 1024], P('data', 'seq'), parts along dimension 0
There are 2 independent parts. The reference program is written for one: setup_inputs(seed, part) draws one part's arguments, and reference() takes and returns one part's arrays. A program takes and returns all parts, laid end to end along the dimension named above; an argument that names none is the same for every part.
All inputs are finite; a program needn't handle non-finite values.
Results may differ from the reference program's by a relative error of at most 0.0141482.
Values are sent between devices in bfloat16 or wider.
A program may use at most 1 GiB of HBM per device.

```python
import math
import jax
import jax.numpy as jnp
from jax import lax

D_MODEL = 1024
SSD_HEADS = 24
SSD_HEAD_DIM = 64
D_STATE = 128
Q_HEADS = 8
KV_HEADS = 2
HEAD_DIM = 64
FF_DIM = 2048
TOK_DEV = 256
SEQ_LEN = 1024
BATCH_SIZE = 2
SSD_BLOCK = 64
NORM_EPS = 1e-6
ROPE_BASE = 10000.0
INNER = SSD_HEADS * SSD_HEAD_DIM
IN_WIDTH = 2 * INNER + 2 * D_STATE + SSD_HEADS
GROUP_SIZE = Q_HEADS // KV_HEADS
N_SSD_BLOCKS = SEQ_LEN // SSD_BLOCK
N_ATTN_BLOCKS = SEQ_LEN // TOK_DEV


def setup_inputs(seed: int = 0, part: int = 0) -> dict:
    base_key = jax.random.key(seed)
    part_key = jax.random.fold_in(base_key, part)
    key_list = jax.random.split(base_key, 12)
    in_scale = D_MODEL ** -0.5
    bc_scale = in_scale * 1.4 * (D_STATE * TOK_DEV) ** -0.25
    q_scale = in_scale * math.sqrt(max(math.log(SEQ_LEN / 32.0), 1.0))
    col_scale = jnp.concatenate([jnp.full((2 * INNER,), in_scale, jnp.float32), jnp.full((2 * D_STATE,), bc_scale, jnp.float32), jnp.full((SSD_HEADS,), 0.5 * in_scale, jnp.float32)])
    w_in = (jax.random.normal(key_list[0], (D_MODEL, IN_WIDTH), jnp.float32) * col_scale).astype(jnp.bfloat16)
    dt_bias = jax.random.uniform(key_list[1], (SSD_HEADS,), jnp.float32, -2.5, -0.5)
    decay_ratio = jnp.exp(jax.random.uniform(key_list[2], (SSD_HEADS,), jnp.float32, math.log(0.15), math.log(1.4)))
    a_neg = -decay_ratio / (TOK_DEV * jax.nn.softplus(dt_bias))
    d_skip = jax.random.uniform(key_list[3], (SSD_HEADS,), jnp.float32, 0.5, 1.5)
    w_out = (jax.random.normal(key_list[4], (INNER, D_MODEL), jnp.float32) * INNER ** -0.5).astype(jnp.bfloat16)
    w_up1 = (jax.random.normal(key_list[5], (D_MODEL, 2 * FF_DIM), jnp.float32) * in_scale).astype(jnp.bfloat16)
    w_down1 = (jax.random.normal(key_list[6], (FF_DIM, D_MODEL), jnp.float32) * FF_DIM ** -0.5).astype(jnp.bfloat16)
    w_q = (jax.random.normal(key_list[7], (D_MODEL, Q_HEADS, HEAD_DIM), jnp.float32) * q_scale).astype(jnp.bfloat16)
    w_kv = (jax.random.normal(key_list[8], (D_MODEL, 2, KV_HEADS, HEAD_DIM), jnp.float32) * in_scale).astype(jnp.bfloat16)
    w_o = (jax.random.normal(key_list[9], (Q_HEADS, HEAD_DIM, D_MODEL), jnp.float32) * (2.0 * (Q_HEADS * HEAD_DIM) ** -0.5)).astype(jnp.bfloat16)
    w_up2 = (jax.random.normal(key_list[10], (D_MODEL, 2 * FF_DIM), jnp.float32) * in_scale).astype(jnp.bfloat16)
    w_down2 = (jax.random.normal(key_list[11], (FF_DIM, D_MODEL), jnp.float32) * FF_DIM ** -0.5).astype(jnp.bfloat16)
    x = jax.random.normal(part_key, (BATCH_SIZE, SEQ_LEN, D_MODEL), jnp.float32).astype(jnp.bfloat16)
    return {'x': x, 'w_in': w_in, 'dt_bias': dt_bias, 'a_neg': a_neg, 'd_skip': d_skip, 'w_out': w_out, 'w_up1': w_up1, 'w_down1': w_down1, 'w_q': w_q, 'w_kv': w_kv, 'w_o': w_o, 'w_up2': w_up2, 'w_down2': w_down2}


def rms_norm(values):
    values = values.astype(jnp.float32)
    return values * lax.rsqrt(jnp.mean(values * values, axis=-1, keepdims=True) + NORM_EPS)


def ssd_layer(seq_x, w_in, dt_bias, a_neg, d_skip, w_out):
    normed = rms_norm(seq_x).astype(jnp.bfloat16)
    in_proj = jnp.dot(normed, w_in, preferred_element_type=jnp.float32).astype(jnp.bfloat16)
    x_heads = in_proj[:, :INNER].reshape(N_SSD_BLOCKS, SSD_BLOCK, SSD_HEADS, SSD_HEAD_DIM)
    gate_z = in_proj[:, INNER:2 * INNER]
    b_mat = in_proj[:, 2 * INNER:2 * INNER + D_STATE].reshape(N_SSD_BLOCKS, SSD_BLOCK, D_STATE)
    c_mat = in_proj[:, 2 * INNER + D_STATE:2 * INNER + 2 * D_STATE].reshape(N_SSD_BLOCKS, SSD_BLOCK, D_STATE)
    dt_val = jax.nn.softplus(in_proj[:, 2 * INNER + 2 * D_STATE:].astype(jnp.float32) + dt_bias)
    log_decay = (dt_val * a_neg).reshape(N_SSD_BLOCKS, SSD_BLOCK, SSD_HEADS)
    dt_blocks = dt_val.reshape(N_SSD_BLOCKS, SSD_BLOCK, SSD_HEADS)
    causal_tri = jnp.arange(SSD_BLOCK)[:, None] >= jnp.arange(SSD_BLOCK)[None, :]

    def block_step(state, blk_args):
        x_blk, b_blk, c_blk, dt_blk, log_blk = blk_args
        cum_log = jnp.cumsum(log_blk, axis=0)
        decay_ts = jnp.exp(jnp.where(causal_tri[:, :, None], cum_log[:, None, :] - cum_log[None, :, :], -jnp.inf))
        scores = jnp.dot(c_blk, b_blk.T, preferred_element_type=jnp.float32)
        mix_mat = (scores[:, :, None] * decay_ts * dt_blk[None, :, :]).astype(jnp.bfloat16)
        x_wide = x_blk.astype(jnp.float32)
        y_intra = jnp.einsum('tsh,shp->thp', mix_mat.astype(jnp.float32), x_wide)
        state_low = state.astype(jnp.bfloat16).astype(jnp.float32)
        y_inter = jnp.exp(cum_log)[:, :, None] * jnp.einsum('tn,hpn->thp', c_blk.astype(jnp.float32), state_low)
        to_end = jnp.exp(cum_log[-1][None, :] - cum_log) * dt_blk
        x_weighted = (x_wide * to_end[:, :, None]).astype(jnp.bfloat16)
        block_state = jnp.einsum('shp,sn->hpn', x_weighted.astype(jnp.float32), b_blk.astype(jnp.float32))
        new_state = jnp.exp(cum_log[-1])[:, None, None] * state + block_state
        return new_state, y_intra + y_inter + d_skip[None, :, None] * x_wide

    init_state = jnp.zeros((SSD_HEADS, SSD_HEAD_DIM, D_STATE), jnp.float32)
    scan_out = lax.scan(block_step, init_state, (x_heads, b_mat, c_mat, dt_blocks, log_decay))
    y_flat = scan_out[1].reshape(SEQ_LEN, INNER)
    gated = (rms_norm(y_flat) * jax.nn.silu(gate_z.astype(jnp.float32))).astype(jnp.bfloat16)
    return (seq_x.astype(jnp.float32) + jnp.dot(gated, w_out, preferred_element_type=jnp.float32)).astype(jnp.bfloat16)


def swiglu_mlp(seq_x, w_up, w_down):
    normed = rms_norm(seq_x).astype(jnp.bfloat16)
    hidden = jnp.dot(normed, w_up, preferred_element_type=jnp.float32)
    gated_act = (jax.nn.silu(hidden[:, :FF_DIM]) * hidden[:, FF_DIM:]).astype(jnp.bfloat16)
    return (seq_x.astype(jnp.float32) + jnp.dot(gated_act, w_down, preferred_element_type=jnp.float32)).astype(jnp.bfloat16)


def rope_tables(positions):
    half_dim = HEAD_DIM // 2
    inv_freq = ROPE_BASE ** (-(jnp.arange(half_dim, dtype=jnp.float32) * 2.0 / HEAD_DIM))
    angles = positions.astype(jnp.float32)[:, None] * inv_freq[None, :]
    return jnp.cos(angles), jnp.sin(angles)


def apply_rope(values, cos_t, sin_t):
    half_dim = HEAD_DIM // 2
    first_half = values[..., :half_dim]
    second_half = values[..., half_dim:]
    cos_b = cos_t[:, None, :]
    sin_b = sin_t[:, None, :]
    return jnp.concatenate([first_half * cos_b - second_half * sin_b, second_half * cos_b + first_half * sin_b], axis=-1)


def attention_layer(seq_x, w_q, w_kv, w_o):
    normed = rms_norm(seq_x).astype(jnp.bfloat16)
    q_proj = jnp.dot(normed, w_q.reshape(D_MODEL, Q_HEADS * HEAD_DIM), preferred_element_type=jnp.float32).reshape(SEQ_LEN, Q_HEADS, HEAD_DIM)
    kv_proj = jnp.dot(normed, w_kv.reshape(D_MODEL, 2 * KV_HEADS * HEAD_DIM), preferred_element_type=jnp.float32).reshape(SEQ_LEN, 2, KV_HEADS, HEAD_DIM)
    cos_t, sin_t = rope_tables(jnp.arange(SEQ_LEN))
    q_rot = apply_rope(q_proj, cos_t, sin_t).astype(jnp.bfloat16)
    k_rot = apply_rope(kv_proj[:, 0], cos_t, sin_t).astype(jnp.bfloat16)
    v_vals = kv_proj[:, 1].astype(jnp.bfloat16)
    q_blocks = q_rot.reshape(N_ATTN_BLOCKS, TOK_DEV, KV_HEADS, GROUP_SIZE, HEAD_DIM).astype(jnp.float32)
    k_blocks = k_rot.reshape(N_ATTN_BLOCKS, TOK_DEV, KV_HEADS, HEAD_DIM).astype(jnp.float32)
    v_blocks = v_vals.reshape(N_ATTN_BLOCKS, TOK_DEV, KV_HEADS, HEAD_DIM).astype(jnp.float32)
    offsets = jnp.arange(TOK_DEV)
    attn_scale = HEAD_DIM ** -0.5

    def one_query_block(q_args):
        q_idx, q_blk = q_args

        def kv_step(acc_state, kv_args):
            k_idx, k_blk, v_blk = kv_args

            def visit_block(old_state):
                run_max, run_sum, acc_vals = old_state
                scores = jnp.einsum('qkgd,skd->kgqs', q_blk, k_blk) * attn_scale
                visible = (q_idx * TOK_DEV + offsets)[:, None] >= (k_idx * TOK_DEV + offsets)[None, :]
                scores = jnp.where(visible, scores, -jnp.inf)
                new_max = jnp.maximum(run_max, jnp.max(scores, axis=-1))
                correction = jnp.exp(run_max - new_max)
                prob_vals = jnp.exp(scores - new_max[..., None])
                new_sum = run_sum * correction + jnp.sum(prob_vals, axis=-1)
                new_acc = acc_vals * correction[..., None] + jnp.einsum('kgqs,skd->kgqd', prob_vals.astype(jnp.bfloat16).astype(jnp.float32), v_blk)
                return new_max, new_sum, new_acc

            return lax.cond(k_idx <= q_idx, visit_block, lambda old_state: old_state, acc_state), None

        stat_shape = (KV_HEADS, GROUP_SIZE, TOK_DEV)
        init_state = (jnp.full(stat_shape, -jnp.inf, jnp.float32), jnp.zeros(stat_shape, jnp.float32), jnp.zeros(stat_shape + (HEAD_DIM,), jnp.float32))
        scan_out = lax.scan(kv_step, init_state, (jnp.arange(N_ATTN_BLOCKS), k_blocks, v_blocks))
        final_state = scan_out[0]
        return (final_state[2] / final_state[1][..., None]).astype(jnp.bfloat16)

    block_outs = lax.map(one_query_block, (jnp.arange(N_ATTN_BLOCKS), q_blocks))
    attn_vals = block_outs.transpose(0, 3, 1, 2, 4).reshape(SEQ_LEN, Q_HEADS * HEAD_DIM)
    attn_out = jnp.dot(attn_vals, w_o.reshape(Q_HEADS * HEAD_DIM, D_MODEL), preferred_element_type=jnp.float32)
    return (seq_x.astype(jnp.float32) + attn_out).astype(jnp.bfloat16)


def reference(x, w_in, dt_bias, a_neg, d_skip, w_out, w_up1, w_down1, w_q, w_kv, w_o, w_up2, w_down2):
    def one_sequence(seq_x):
        hidden = ssd_layer(seq_x, w_in, dt_bias, a_neg, d_skip, w_out)
        hidden = swiglu_mlp(hidden, w_up1, w_down1)
        hidden = attention_layer(hidden, w_q, w_kv, w_o)
        return swiglu_mlp(hidden, w_up2, w_down2)

    return lax.map(one_sequence, x)
```

```python
import functools
import jax
import jax.numpy as jnp
import numpy as np
from jax import lax
from jax.experimental import pallas as pl
from jax.experimental.pallas import tpu as pltpu
from jax.sharding import PartitionSpec as P

F32 = jnp.float32
BF16 = jnp.bfloat16
BLK = 64
EPS = 1e-6
ROPE_BASE = 10000.0
NSEQ = 2
TOK = 256
NBLK = TOK // BLK
ROWS = NSEQ * TOK
D = 1024
INNER = 1536
HEADS = 24
NST = 128
FF = 2048
NCH = 3
CHW = INNER // NCH
GW = 256
HD = 64
QH = 8


def dot(a, b):
    return jnp.dot(a, b, preferred_element_type=F32)


def dot_t(a, b):
    return lax.dot_general(a, b, (((1,), (1,)), ((), ())), preferred_element_type=F32)


def hdot(a, b):
    return jnp.dot(a, b, preferred_element_type=F32, precision=lax.Precision.HIGHEST)


def iota(shape, dim):
    return lax.broadcasted_iota(jnp.int32, shape, dim)


def split3(v, lane):
    hi = v.astype(BF16)
    rest = v - hi.astype(F32)
    mid = rest.astype(BF16)
    low = rest - mid.astype(F32)
    return jnp.where(lane < 32, hi.astype(F32), jnp.where(lane < 64, mid.astype(F32), low)).astype(BF16)


def silu(v):
    return v * jax.nn.sigmoid(v)


def kernel(x_h, win_h, bias_r, aneg_r, dskip_r, wout_h, up1_h, down1_h, wq_h, wkv_h, wo_h, up2_h, down2_h, cos_h, sin_h, out_h,
           x_v, u_v, wx_v, wz_v, wt_v, wout_v, up_v, down_v, wq_v, wkv_v, wo_v, cos_v, sin_v,
           xs_v, z_v, b_v, c_v, csp_v, dsp_v, e4_v, bd_v, y_v, ec_v, el_v, dsk_v, bs_v, e_v, hin_v, act_v,
           q_v, kv_v, vt_v, m_v, l_v, acc_v, att_v,
           lsem, osem, st_ssem, st_rsem, k_ssem, k_rsem, v_ssem, v_rsem):
    me = lax.axis_index('seq')
    copies = {}

    def load(name, src, dst, idx):
        copies[name] = pltpu.make_async_copy(src, dst, lsem.at[idx])
        copies[name].start()

    load('x', x_h, x_v, 0)
    load('wx', win_h.at[:, pl.ds(0, INNER)], wx_v, 1)
    load('wt', win_h.at[:, pl.ds(2 * INNER, 2 * NST + HEADS)], wt_v, 2)

    barrier = pltpu.get_barrier_semaphore()
    for off in (1, 2, 3):
        pl.semaphore_signal(barrier, inc=1, device_id={'seq': lax.rem(me + off, 4)}, device_id_type=pl.DeviceIdType.MESH)

    spread = ((iota((HEADS, 128), 1) & 31) == iota((HEADS, 128), 0)) & (iota((HEADS, 128), 1) < 96)
    spread = spread.astype(F32)
    lane8 = iota((8, 128), 1)
    bias3 = hdot(jnp.broadcast_to(bias_r[...], (8, HEADS)), spread)[0:1]
    aneg3 = hdot(jnp.broadcast_to(aneg_r[...], (8, HEADS)), spread)[0:1]
    dsk3 = split3(hdot(jnp.broadcast_to(dskip_r[...], (8, HEADS)), spread), lane8)
    for g in range(INNER // GW):
        cols = pl.ds(g * GW, GW)
        head = (iota((128, GW), 1) + g * GW) >> 6
        row = iota((128, GW), 0)
        e4_v[:, cols] = (((row & 31) == head) & (row < 96)).astype(F32).astype(BF16)
        dsk_v[:, cols] = dot(dsk3, e4_v[:, cols])
    bd_v[...] = ((iota((GW, GW), 0) >> 6) == (iota((GW, GW), 1) >> 6)).astype(F32).astype(BF16)
    for s in range(NSEQ):
        for ch in range(NCH):
            e_v[s, ch] = jnp.zeros((NST, CHW), F32)

    @pl.when(me == 0)
    def _():
        for s in range(NSEQ):
            for ch in range(NCH):
                hin_v[s, ch] = jnp.zeros((NST, CHW), F32)

    def norm_rows(start, count):
        def body(step, carry):
            rows = pl.ds(pl.multiple_of(start + step * 64, 64), 64)
            vals = x_v[rows, :].astype(F32)
            scale = lax.rsqrt(jnp.mean(vals * vals, axis=-1, keepdims=True) + EPS)
            u_v[rows, :] = (vals * scale).astype(BF16)
            return carry
        lax.fori_loop(0, count // 64, body, 0)

    copies['x'].wait()
    norm_rows(0, ROWS)
    load('wz', win_h.at[:, pl.ds(INNER, INNER)], wz_v, 3)
    copies['wx'].wait()
    copies['wt'].wait()
    load('wout', wout_h, wout_v, 4)
    load('up', up1_h, up_v, 5)

    tail = dot(u_v[...], wt_v[...])
    b_v[...] = tail[:, :NST].astype(BF16)
    c_v[...] = tail[:, NST:2 * NST].astype(BF16)
    r_bf = tail[:, 2 * NST:].astype(BF16)
    spread_bf = spread.astype(BF16)
    tri = (iota((TOK, TOK), 0) >= iota((TOK, TOK), 1)) & ((iota((TOK, TOK), 0) >> 6) == (iota((TOK, TOK), 1) >> 6))
    tri = tri.astype(F32)
    lane = iota((TOK, 128), 1)
    for s in range(NSEQ):
        pre = dot(r_bf[s * TOK:(s + 1) * TOK], spread_bf) + bias3
        dt = jnp.maximum(pre, 0.0) + jnp.log1p(jnp.exp(-jnp.abs(pre)))
        cum = hdot(tri, dt * aneg3)
        csp_v[s * TOK:(s + 1) * TOK, :] = split3(cum, lane)
        dsp_v[s * TOK:(s + 1) * TOK, :] = split3(dt, lane)

    def proj_x(j, carry):
        cols = pl.ds(pl.multiple_of(j * 512, 512), 512)
        xs_v[:, cols] = dot(u_v[...], wx_v[:, cols]).astype(BF16)
        return carry
    lax.fori_loop(0, INNER // 512, proj_x, 0)

    t_idx = iota((BLK, GW), 0)
    s_idx = iota((BLK, GW), 1) & (BLK - 1)

    def block_step(s):
        def body(b, carry):
            i = s * NBLK + b
            rows = pl.ds(pl.multiple_of(i * BLK, BLK), BLK)
            cs = csp_v[rows, :]
            ds = dsp_v[rows, :]
            bb = b_v[rows, :]
            cb = c_v[rows, :]
            b4 = jnp.concatenate([bb] * 4, axis=0)
            sc4 = dot_t(cb, b4)
            bt = bb.astype(F32).T.astype(BF16)
            for g in range(INNER // GW):
                ch, off = g // 2, (g % 2) * GW
                cols = pl.ds(g * GW, GW)
                ce = dot(cs, e4_v[:, cols])
                de = dot(ds, e4_v[:, cols])
                crow = jnp.sum(jnp.where(t_idx == s_idx, ce, 0.0), axis=0, keepdims=True)
                drow = jnp.sum(jnp.where(t_idx == s_idx, de, 0.0), axis=0, keepdims=True)
                decay = jnp.exp(jnp.where(t_idx >= s_idx, ce - crow, -jnp.inf))
                mix = (sc4 * decay * drow).astype(BF16)
                xg = xs_v[rows, cols]
                xw = xg.astype(F32)
                xbd = jnp.concatenate([xg] * 4, axis=0) * bd_v[...]
                y_v[rows, cols] = dot(mix, xbd) + dsk_v[0:1, cols] * xw
                last = ce[BLK - 1:BLK, :]
                to_end = jnp.exp(last - ce) * de
                state = dot(bt, (xw * to_end).astype(BF16))
                el = jnp.exp(last)
                bs_v[i, ch, :, off:off + GW] = state
                ec_v[rows, cols] = jnp.exp(ce)
                el_v[pl.ds(pl.multiple_of(i * 8, 8), 8), cols] = jnp.broadcast_to(el, (8, GW))
                e_v[s, ch, :, off:off + GW] = el * e_v[s, ch, :, off:off + GW] + state
            return carry
        return body

    def st_copy(s, ch, dst):
        src = e_v.at[s, ch]
        return pltpu.make_async_remote_copy(src_ref=src, dst_ref=hin_v.at[s, ch], send_sem=st_ssem.at[s, ch], recv_sem=st_rsem.at[s, ch],
                                            device_id={'seq': dst}, device_id_type=pl.DeviceIdType.MESH)

    def chain(s, ch, dst):
        cols = pl.ds(ch * CHW, CHW)
        total = el_v[(s * NBLK) * 8:(s * NBLK) * 8 + 1, cols]
        for b in range(1, NBLK):
            total = total * el_v[(s * NBLK + b) * 8:(s * NBLK + b) * 8 + 1, cols]
        e_v[s, ch] = total * hin_v[s, ch] + e_v[s, ch]
        st_copy(s, ch, dst).start()

    def first_send(s):
        @pl.when(me == 0)
        def _():
            for ch in range(NCH):
                st_copy(s, ch, 1).start()

    def relay(s):
        @pl.when(me == 1)
        def _():
            for ch in range(NCH):
                st_copy(s, ch, 2).wait_recv()
                chain(s, ch, 2)

    lax.fori_loop(0, NBLK, block_step(0), 0)
    pl.semaphore_wait(barrier, 3)
    first_send(0)
    lax.fori_loop(0, NBLK // 2, block_step(1), 0)
    relay(0)
    lax.fori_loop(NBLK // 2, NBLK, block_step(1), 0)
    first_send(1)
    load('down', down1_h, down_v, 6)
    load('wq', wq_h, wq_v, 7)
    load('wkv', wkv_h, wkv_v, 8)
    load('wo', wo_h, wo_v, 9)
    tab = pl.ds(pl.multiple_of(me * TOK, TOK), TOK)
    load('cos', cos_h.at[tab, :], cos_v, 10)
    load('sin', sin_h.at[tab, :], sin_v, 11)
    copies['wz'].wait()

    def proj_z(j, carry):
        cols = pl.ds(pl.multiple_of(j * 512, 512), 512)
        z_v[:, cols] = dot(u_v[...], wz_v[:, cols]).astype(BF16)
        return carry
    lax.fori_loop(0, INNER // 512, proj_z, 0)
    relay(1)

    def ssd_finish(s):
        @pl.when(me == 1)
        def _():
            pass

        @pl.when(me == 2)
        def _():
            for ch in range(NCH):
                st_copy(s, ch, 3).wait_recv()
                chain(s, ch, 3)

        @pl.when(me == 3)
        def _():
            for ch in range(NCH):
                st_copy(s, ch, 3).wait_recv()

        def body(b, carry):
            i = s * NBLK + b
            rows = pl.ds(pl.multiple_of(i * BLK, BLK), BLK)
            cb = c_v[rows, :]
            for ch in range(NCH):
                cols = pl.ds(ch * CHW, CHW)
                held = hin_v[s, ch]
                y_v[rows, cols] = y_v[rows, cols] + ec_v[rows, cols] * dot(cb, held.astype(BF16))
                el = el_v[pl.ds(pl.multiple_of(i * 8, 8), 8), cols][0:1]
                hin_v[s, ch] = el * held + bs_v[i, ch]
            ssq = jnp.zeros((BLK, 1), F32)
            for ch in range(NCH):
                yv = y_v[rows, ch * CHW:(ch + 1) * CHW]
                ssq = ssq + jnp.sum(yv * yv, axis=-1, keepdims=True)
            scale = lax.rsqrt(ssq * (1.0 / INNER) + EPS)
            for ch in range(NCH):
                cols = pl.ds(ch * CHW, CHW)
                xs_v[rows, cols] = (y_v[rows, cols] * scale * silu(z_v[rows, cols].astype(F32))).astype(BF16)
            return carry
        lax.fori_loop(0, NBLK, body, 0)

        rows = pl.ds(s * TOK, TOK)

        def out_proj(j, carry):
            cols = pl.ds(pl.multiple_of(j * 512, 512), 512)
            x_v[rows, cols] = (x_v[rows, cols].astype(F32) + dot(xs_v[rows, :], wout_v[:, cols])).astype(BF16)
            return carry
        lax.fori_loop(0, D // 512, out_proj, 0)

    def mlp_up(start, count, width):
        rows = pl.ds(start, count)

        def body(j, carry):
            c0 = pl.multiple_of(j * width, width)
            gate = dot(u_v[rows, :], up_v[:, pl.ds(c0, width)])
            up = dot(u_v[rows, :], up_v[:, pl.ds(FF + c0, width)])
            act_v[rows, pl.ds(c0, width)] = (silu(gate) * up).astype(BF16)
            return carry
        lax.fori_loop(0, FF // width, body, 0)

    def mlp_down(start, count, width):
        rows = pl.ds(start, count)

        def body(j, carry):
            cols = pl.ds(pl.multiple_of(j * width, width), width)
            x_v[rows, cols] = (x_v[rows, cols].astype(F32) + dot(act_v[rows, :], down_v[:, cols])).astype(BF16)
            return carry
        lax.fori_loop(0, D // width, body, 0)

    def rope(vals):
        low = (iota(vals.shape, 1) & 63) < 32
        swapped = jnp.where(low, pltpu.roll(vals, 96, 1), pltpu.roll(vals, 32, 1))
        return vals * cos_v[...] + swapped * sin_v[...]

    def k_copy(s, piece, slot, dst):
        return pltpu.make_async_remote_copy(src_ref=kv_v.at[s, piece], dst_ref=kv_v.at[s, piece], send_sem=k_ssem.at[s, slot], recv_sem=k_rsem.at[s, piece],
                                            device_id={'seq': dst}, device_id_type=pl.DeviceIdType.MESH)

    def v_copy(s, piece, slot, dst):
        return pltpu.make_async_remote_copy(src_ref=vt_v.at[s, piece], dst_ref=vt_v.at[s, piece], send_sem=v_ssem.at[s, slot], recv_sem=v_rsem.at[s, piece],
                                            device_id={'seq': dst}, device_id_type=pl.DeviceIdType.MESH)

    def kv_send(s, piece, slot, dst):
        k_copy(s, piece, slot, dst).start()
        v_copy(s, piece, slot, dst).start()

    def kv_wait(s, piece):
        k_copy(s, piece, 0, 0).wait_recv()
        v_copy(s, piece, 0, 0).wait_recv()

    def kv_sent(s, piece, slot, dst):
        k_copy(s, piece, slot, dst).wait_send()
        v_copy(s, piece, slot, dst).wait_send()

    def qkv(s):
        rows = pl.ds(s * TOK, TOK)
        norm_rows(s * TOK, TOK)
        kv = dot(u_v[rows, :], wkv_v[...])
        kv_v[s, me] = rope(kv[:, :128]).astype(BF16)
        vt_v[s, me] = kv[:, 128:].T.astype(BF16)
        q = dot(u_v[rows, :], wq_v[...])
        for pair in range(QH // 2):
            rot = rope(q[:, pair * 128:(pair + 1) * 128]).astype(BF16)
            q_v[2 * pair] = rot[:, :HD]
            q_v[2 * pair + 1] = rot[:, HD:]

        @pl.when(me == 0)
        def _():
            kv_send(s, 0, 0, 1)
            kv_send(s, 0, 1, 2)

        @pl.when(me == 1)
        def _():
            kv_send(s, 1, 0, 3)

        @pl.when(me == 2)
        def _():
            kv_send(s, 2, 0, 3)
            kv_wait(s, 0)
            kv_send(s, 0, 1, 3)

        @pl.when(me == 3)
        def _():
            kv_wait(s, 1)
            kv_send(s, 1, 0, 2)

    def attend(s, piece, first):
        causal = iota((TOK, TOK), 0) <= iota((TOK, TOK), 1)
        keys = kv_v[s, piece]
        vals = vt_v[s, piece]
        for h in range(QH):
            g = h // 4
            k_g = keys[:, g * HD:(g + 1) * HD]
            v_g = vals[g * HD:(g + 1) * HD, :]
            sc = dot_t(k_g, q_v[h]) * 0.125
            if first:
                sc = jnp.where(causal, sc, -jnp.inf)
                top = jnp.max(sc, axis=0, keepdims=True)
                prob = jnp.exp(sc - top)
                l_v[h:h + 1, :] = jnp.sum(prob, axis=0, keepdims=True)
                acc_v[h] = dot(v_g, prob.astype(BF16))
            else:
                old = m_v[h:h + 1, :]
                top = jnp.maximum(old, jnp.max(sc, axis=0, keepdims=True))
                fix = jnp.exp(old - top)
                prob = jnp.exp(sc - top)
                l_v[h:h + 1, :] = l_v[h:h + 1, :] * fix + jnp.sum(prob, axis=0, keepdims=True)
                acc_v[h] = acc_v[h] * fix + dot(v_g, prob.astype(BF16))
            m_v[h:h + 1, :] = top

    def attention(s):
        attend(s, me, True)
        for piece in range(3):
            @pl.when(me > piece)
            def _(piece=piece):
                if piece == 0:
                    @pl.when(me != 2)
                    def _():
                        kv_wait(s, 0)
                elif piece == 1:
                    @pl.when(me == 2)
                    def _():
                        kv_wait(s, 1)
                else:
                    kv_wait(s, 2)
                attend(s, piece, False)
        rows = pl.ds(s * TOK, TOK)
        for pair in range(QH // 2):
            top = acc_v[2 * pair] / l_v[2 * pair:2 * pair + 1, :]
            bot = acc_v[2 * pair + 1] / l_v[2 * pair + 1:2 * pair + 2, :]
            att_v[:, pair * 128:(pair + 1) * 128] = jnp.concatenate([top, bot], axis=0).T.astype(BF16)

        def o_proj(j, carry):
            cols = pl.ds(pl.multiple_of(j * 512, 512), 512)
            x_v[rows, cols] = (x_v[rows, cols].astype(F32) + dot(att_v[...], wo_v[:, cols])).astype(BF16)
            return carry
        lax.fori_loop(0, D // 512, o_proj, 0)

    copies['wout'].wait()
    ssd_finish(0)
    norm_rows(0, TOK)
    copies['up'].wait()
    mlp_up(0, TOK, 512)
    copies['down'].wait()
    mlp_down(0, TOK, 512)
    for name in ('wq', 'wkv', 'wo', 'cos', 'sin'):
        copies[name].wait()
    qkv(0)
    attention(0)
    ssd_finish(1)
    norm_rows(TOK, TOK)
    mlp_up(TOK, TOK, 512)
    load('up', up2_h, up_v, 5)
    mlp_down(TOK, TOK, 512)
    load('down', down2_h, down_v, 6)
    qkv(1)
    attention(1)
    norm_rows(0, ROWS)
    copies['up'].wait()
    mlp_up(0, ROWS, 256)
    copies['down'].wait()
    mlp_down(0, ROWS, 256)
    done = pltpu.make_async_copy(x_v, out_h, osem)
    done.start()

    @pl.when(me < 3)
    def _():
        for s in range(NSEQ):
            for ch in range(NCH):
                st_copy(s, ch, 0).wait_send()
    for s in range(NSEQ):
        kv_sent(s, 0, 0, 0)

        @pl.when((me == 0) | (me == 2))
        def _():
            kv_sent(s, 0, 1, 0)
    done.wait()


def rope_tables(seq_len):
    inv = (np.float32(ROPE_BASE) ** (-(np.arange(32, dtype=np.float32) * np.float32(2.0) / np.float32(HD)))).astype(np.float32)
    ang = (np.arange(seq_len, dtype=np.float32)[:, None] * inv[None, :]).astype(np.float32).astype(np.float64)
    cos = np.cos(ang).astype(np.float32)
    sin = np.sin(ang).astype(np.float32)
    return np.tile(cos, (1, 4)), np.concatenate([-sin, sin, -sin, sin], axis=1)


def solution(mesh):
    n_dev = mesh.shape['seq']
    cos_t, sin_t = rope_tables(n_dev * TOK)
    any_spec = pl.BlockSpec(memory_space=pl.ANY)
    vm_spec = pl.BlockSpec(memory_space=pltpu.VMEM)
    vm = pltpu.VMEM
    call = pl.pallas_call(
        kernel,
        out_shape=jax.ShapeDtypeStruct((ROWS, D), BF16),
        in_specs=[any_spec, any_spec, vm_spec, vm_spec, vm_spec] + [any_spec] * 10,
        out_specs=any_spec,
        scratch_shapes=[
            vm((ROWS, D), BF16), vm((ROWS, D), BF16), vm((D, INNER), BF16), vm((D, INNER), BF16), vm((D, 2 * NST + HEADS), BF16),
            vm((INNER, D), BF16), vm((D, 2 * FF), BF16), vm((FF, D), BF16), vm((D, QH * HD), BF16), vm((D, 256), BF16), vm((QH * HD, D), BF16),
            vm((TOK, 128), F32), vm((TOK, 128), F32),
            vm((ROWS, INNER), BF16), vm((ROWS, INNER), BF16), vm((ROWS, NST), BF16), vm((ROWS, NST), BF16),
            vm((ROWS, 128), BF16), vm((ROWS, 128), BF16), vm((128, INNER), BF16), vm((GW, GW), BF16),
            vm((ROWS, INNER), F32), vm((ROWS, INNER), F32), vm((NSEQ * NBLK * 8, INNER), F32), vm((8, INNER), F32),
            vm((NSEQ * NBLK, NCH, NST, CHW), F32), vm((NSEQ, NCH, NST, CHW), F32), vm((NSEQ, NCH, NST, CHW), F32), vm((ROWS, FF), BF16),
            vm((QH, TOK, HD), BF16), vm((NSEQ, 4, TOK, 128), BF16), vm((NSEQ, 4, 128, TOK), BF16),
            vm((QH, TOK), F32), vm((QH, TOK), F32), vm((QH, HD, TOK), F32), vm((TOK, QH * HD), BF16),
            pltpu.SemaphoreType.DMA((12,)), pltpu.SemaphoreType.DMA, pltpu.SemaphoreType.DMA((NSEQ, NCH)), pltpu.SemaphoreType.DMA((NSEQ, NCH)),
            pltpu.SemaphoreType.DMA((NSEQ, 2)), pltpu.SemaphoreType.DMA((NSEQ, 4)), pltpu.SemaphoreType.DMA((NSEQ, 2)), pltpu.SemaphoreType.DMA((NSEQ, 4)),
        ],
        compiler_params=pltpu.CompilerParams(collective_id=0, has_side_effects=True, vmem_limit_bytes=67_000_000),
        name='layer_stack',
    )

    def local_fn(x_loc, w_in, dt_bias, a_neg, d_skip, w_out, w_up1, w_down1, w_q, w_kv, w_o, w_up2, w_down2):
        out = call(x_loc.reshape(ROWS, D), w_in, dt_bias.reshape(1, HEADS), a_neg.reshape(1, HEADS), d_skip.reshape(1, HEADS), w_out, w_up1, w_down1,
                   w_q.reshape(D, QH * HD), w_kv.reshape(D, 256), w_o.reshape(QH * HD, D), w_up2, w_down2, jnp.asarray(cos_t), jnp.asarray(sin_t))
        return out.reshape(x_loc.shape)

    seq_spec = P('data', 'seq', None)
    return jax.shard_map(local_fn, mesh=mesh, in_specs=(seq_spec,) + (P(),) * 12, out_specs=seq_spec, check_vma=False)
```

```python
import functools
import jax
import jax.numpy as jnp
import numpy as np
from jax import lax
from jax.experimental import pallas as pl
from jax.experimental.pallas import tpu as pltpu
from jax.sharding import PartitionSpec as P

F32 = jnp.float32
BF16 = jnp.bfloat16
BLK = 64
EPS = 1e-6
ROPE_BASE = 10000.0
NSEQ = 2
TOK = 256
NBLK = TOK // BLK
ROWS = NSEQ * TOK
D = 1024
INNER = 1536
HEADS = 24
NST = 128
FF = 2048
NCH = 3
CHW = INNER // NCH
GW = 256
HD = 64
QH = 8


def dot(a, b):
    return jnp.dot(a, b, preferred_element_type=F32)


def dot_t(a, b):
    return lax.dot_general(a, b, (((1,), (1,)), ((), ())), preferred_element_type=F32)


def hdot(a, b):
    return jnp.dot(a, b, preferred_element_type=F32, precision=lax.Precision.HIGHEST)


def iota(shape, dim):
    return lax.broadcasted_iota(jnp.int32, shape, dim)


def split3(v, lane):
    hi = v.astype(BF16)
    rest = v - hi.astype(F32)
    mid = rest.astype(BF16)
    low = rest - mid.astype(F32)
    return jnp.where(lane < 32, hi.astype(F32), jnp.where(lane < 64, mid.astype(F32), low)).astype(BF16)


def silu(v):
    return v * jax.nn.sigmoid(v)


def kernel(x_h, win_h, bias_r, aneg_r, dskip_r, wout_h, up1_h, down1_h, wq_h, wkv_h, wo_h, up2_h, down2_h, cos_h, sin_h, out_h,
           x_v, u_v, wx_v, wz_v, wt_v, wout_v, up_v, down_v, wqkv_v, wo_v, cos_v, sin_v,
           xs_v, z_v, b_v, c_v, csp_v, dsp_v, e4_v, bd_v, y_v, ec_v, de_v, el_v, dsk_v, bs_v, e_v, hin_v, act_v,
           qz_v, kv_v, vt_v, m_v, l_v, acc_v, att_v, sc_v, pr_v,
           lsem, osem, st_ssem, st_rsem, k_ssem, k_rsem, v_ssem, v_rsem):
    me = lax.axis_index('seq')
    copies = {}

    def load(name, src, dst, idx):
        copies[name] = pltpu.make_async_copy(src, dst, lsem.at[idx])
        copies[name].start()

    load('x', x_h, x_v, 0)
    load('wt', win_h.at[pl.ds(2 * INNER, 2 * NST + HEADS), :], wt_v, 1)
    for ch in range(NCH):
        load('wx%d' % ch, win_h.at[pl.ds(ch * CHW, CHW), :], wx_v.at[pl.ds(ch * CHW, CHW), :], 2 + ch)
    load('wz', win_h.at[pl.ds(INNER, INNER), :], wz_v, 5)

    barrier = pltpu.get_barrier_semaphore()
    for off in (1, 2, 3):
        pl.semaphore_signal(barrier, inc=1, device_id={'seq': lax.rem(me + off, 4)}, device_id_type=pl.DeviceIdType.MESH)

    spread = ((iota((HEADS, 128), 1) & 31) == iota((HEADS, 128), 0)) & (iota((HEADS, 128), 1) < 96)
    spread = spread.astype(F32)
    lane8 = iota((8, 128), 1)
    bias3 = hdot(jnp.broadcast_to(bias_r[...], (8, HEADS)), spread)[0:1]
    aneg3 = hdot(jnp.broadcast_to(aneg_r[...], (8, HEADS)), spread)[0:1]
    dsk3 = split3(hdot(jnp.broadcast_to(dskip_r[...], (8, HEADS)), spread), lane8)
    for g in range(INNER // GW):
        cols = pl.ds(g * GW, GW)
        head = (iota((128, GW), 1) + g * GW) >> 6
        row = iota((128, GW), 0)
        e4_v[:, cols] = (((row & 31) == head) & (row < 96)).astype(F32).astype(BF16)
        dsk_v[:, cols] = dot(dsk3, e4_v[:, cols])
    bd_v[...] = ((iota((GW, GW), 0) >> 6) == (iota((GW, GW), 1) >> 6)).astype(F32).astype(BF16)
    for h in range(QH):
        qz_v[h] = jnp.zeros((2 * HD, TOK), BF16)

    @pl.when(me == 0)
    def _():
        for s in range(NSEQ):
            for ch in range(NCH):
                hin_v[s, ch] = jnp.zeros((NST, CHW), F32)

    def norm_rows(start, count):
        def body(step, carry):
            rows = pl.ds(pl.multiple_of(start + step * 128, 128), 128)
            vals = x_v[rows, :].astype(F32)
            scale = lax.rsqrt(jnp.mean(vals * vals, axis=-1, keepdims=True) + EPS)
            u_v[rows, :] = (x_v[rows, :].astype(F32) * scale).astype(BF16)
            return carry
        lax.fori_loop(0, count // 128, body, 0)

    copies['x'].wait()
    norm_rows(0, ROWS)
    copies['wt'].wait()
    copies['wx0'].wait()

    tail = dot_t(u_v[...], wt_v[...])
    b_v[...] = tail[:, :NST].astype(BF16)
    c_v[...] = tail[:, NST:2 * NST].astype(BF16)
    r_bf = tail[:, 2 * NST:].astype(BF16)
    spread_bf = spread.astype(BF16)
    tri = (iota((TOK, TOK), 0) >= iota((TOK, TOK), 1)) & ((iota((TOK, TOK), 0) >> 6) == (iota((TOK, TOK), 1) >> 6))
    tri = tri.astype(F32)
    lane = iota((TOK, 128), 1)
    for s in range(NSEQ):
        pre = dot(r_bf[s * TOK:(s + 1) * TOK], spread_bf) + bias3
        dt = jnp.maximum(pre, 0.0) + jnp.log1p(jnp.exp(-jnp.abs(pre)))
        cum = hdot(tri, dt * aneg3)
        csp_v[s * TOK:(s + 1) * TOK, :] = split3(cum, lane)
        dsp_v[s * TOK:(s + 1) * TOK, :] = split3(dt, lane)

    def proj_x(ch):
        cols = pl.ds(ch * CHW, CHW)
        xs_v[:, cols] = dot_t(u_v[...], wx_v[cols, :]).astype(BF16)

    def head_spread(ch):
        cols = pl.ds(ch * CHW, CHW)
        ec_v[:, cols] = dot(csp_v[...], e4_v[:, cols])
        de_v[:, cols] = dot(dsp_v[...], e4_v[:, cols])

    t_idx = iota((BLK, GW), 0)
    s_idx = iota((BLK, GW), 1) & (BLK - 1)

    def ssd_blocks(s, ch):
        for b in range(NBLK):
            i = s * NBLK + b
            rows = pl.ds(i * BLK, BLK)
            bb = b_v[rows, :]
            sc4 = dot_t(c_v[rows, :], jnp.concatenate([bb] * 4, axis=0))
            bt = bb.astype(F32).T.astype(BF16)
            for half in range(CHW // GW):
                off = half * GW
                cols = pl.ds(ch * CHW + off, GW)
                ce = ec_v[rows, cols]
                de = de_v[rows, cols]
                crow = jnp.sum(jnp.where(t_idx == s_idx, ce, 0.0), axis=0, keepdims=True)
                drow = jnp.sum(jnp.where(t_idx == s_idx, de, 0.0), axis=0, keepdims=True)
                decay = jnp.exp(jnp.where(t_idx >= s_idx, ce - crow, -jnp.inf))
                mix = (sc4 * decay * drow).astype(BF16)
                xg = xs_v[rows, cols]
                xw = xg.astype(F32)
                xbd = jnp.concatenate([xg] * 4, axis=0) * bd_v[...]
                y_v[rows, cols] = dot(mix, xbd) + dsk_v[0:1, cols] * xw
                last = ce[BLK - 1:BLK, :]
                state = dot(bt, (xw * (jnp.exp(last - ce) * de)).astype(BF16))
                el = jnp.exp(last)
                bs_v[i, ch, :, off:off + GW] = state
                ec_v[rows, cols] = jnp.exp(ce)
                el_v[i * 8:i * 8 + 8, cols] = jnp.broadcast_to(el, (8, GW))
                if b == 0:
                    e_v[s, ch, :, off:off + GW] = state
                else:
                    e_v[s, ch, :, off:off + GW] = el * e_v[s, ch, :, off:off + GW] + state

    def st_copy(s, ch, dst):
        return pltpu.make_async_remote_copy(src_ref=e_v.at[s, ch], dst_ref=hin_v.at[s, ch], send_sem=st_ssem.at[s, ch], recv_sem=st_rsem.at[s, ch],
                                            device_id={'seq': dst}, device_id_type=pl.DeviceIdType.MESH)

    def chain(s, ch, dst):
        cols = pl.ds(ch * CHW, CHW)
        total = el_v[(s * NBLK) * 8:(s * NBLK) * 8 + 1, cols]
        for b in range(1, NBLK):
            total = total * el_v[(s * NBLK + b) * 8:(s * NBLK + b) * 8 + 1, cols]
        e_v[s, ch] = total * hin_v[s, ch] + e_v[s, ch]
        st_copy(s, ch, dst).start()

    def first_send(s, ch):
        @pl.when(me == 0)
        def _():
            st_copy(s, ch, 1).start()

    def relay(s, *chunks):
        @pl.when(me == 1)
        def _():
            for ch in chunks:
                st_copy(s, ch, 2).wait_recv()
                chain(s, ch, 2)

    proj_x(0)
    head_spread(0)
    ssd_blocks(0, 0)
    pl.semaphore_wait(barrier, 3)
    first_send(0, 0)
    copies['wx1'].wait()
    load('wout', wout_h, wout_v, 6)
    load('up', up1_h, up_v, 7)
    proj_x(1)
    head_spread(1)
    ssd_blocks(0, 1)
    first_send(0, 1)
    relay(0, 0)
    copies['wx2'].wait()
    proj_x(2)
    head_spread(2)
    ssd_blocks(0, 2)
    first_send(0, 2)
    relay(0, 1)
    load('down', down1_h, down_v, 8)
    load('wq', wq_h, wqkv_v.at[pl.ds(0, QH * HD), :], 9)
    load('wkv', wkv_h, wqkv_v.at[pl.ds(QH * HD, 256), :], 10)
    load('wo', wo_h, wo_v, 11)
    tab = pl.ds(pl.multiple_of(me * TOK, TOK), TOK)
    load('cos', cos_h.at[:, tab], cos_v, 12)
    load('sin', sin_h.at[:, tab], sin_v, 13)
    ssd_blocks(1, 0)
    first_send(1, 0)
    relay(0, 2)
    ssd_blocks(1, 1)
    first_send(1, 1)
    ssd_blocks(1, 2)
    first_send(1, 2)
    relay(1, 0, 1)
    copies['wz'].wait()
    for ch in range(NCH):
        cols = pl.ds(ch * CHW, CHW)
        z_v[:, cols] = dot_t(u_v[...], wz_v[cols, :]).astype(BF16)
    relay(1, 2)

    def ssd_finish(s):
        @pl.when(me == 2)
        def _():
            for ch in range(NCH):
                st_copy(s, ch, 3).wait_recv()
                chain(s, ch, 3)

        @pl.when(me == 3)
        def _():
            for ch in range(NCH):
                st_copy(s, ch, 3).wait_recv()

        for ch in range(NCH):
            cols = pl.ds(ch * CHW, CHW)
            for b in range(NBLK):
                i = s * NBLK + b
                rows = pl.ds(i * BLK, BLK)
                held = hin_v[s, ch]
                y_v[rows, cols] = y_v[rows, cols] + ec_v[rows, cols] * dot(c_v[rows, :], held.astype(BF16))
                if b < NBLK - 1:
                    hin_v[s, ch] = el_v[i * 8:i * 8 + 1, cols] * held + bs_v[i, ch]

        def gate(b, carry):
            rows = pl.ds(pl.multiple_of(s * TOK + b * BLK, BLK), BLK)
            ssq = jnp.zeros((BLK, 1), F32)
            for ch in range(NCH):
                yv = y_v[rows, ch * CHW:(ch + 1) * CHW]
                ssq = ssq + jnp.sum(yv * yv, axis=-1, keepdims=True)
            scale = lax.rsqrt(ssq * (1.0 / INNER) + EPS)
            for ch in range(NCH):
                cols = pl.ds(ch * CHW, CHW)
                xs_v[rows, cols] = (y_v[rows, cols] * scale * silu(z_v[rows, cols].astype(F32))).astype(BF16)
            return carry
        lax.fori_loop(0, NBLK, gate, 0, unroll=2)

        rows = pl.ds(s * TOK, TOK)
        for j in range(D // 512):
            cols = pl.ds(j * 512, 512)
            x_v[rows, cols] = (x_v[rows, cols].astype(F32) + dot(xs_v[rows, :], wout_v[:, cols])).astype(BF16)

    def mlp_up(start, count, width, per_step):
        rows = pl.ds(start, count)

        def body(j, carry):
            for k in range(per_step):
                c0 = pl.multiple_of((j * per_step + k) * width, width)
                gate = dot(u_v[rows, :], up_v[:, pl.ds(c0, width)])
                up = dot(u_v[rows, :], up_v[:, pl.ds(FF + c0, width)])
                act_v[rows, pl.ds(c0, width)] = (silu(gate) * up).astype(BF16)
            return carry
        lax.fori_loop(0, FF // (width * per_step), body, 0)

    def mlp_down(start, count, width, out_copy=None):
        rows = pl.ds(start, count)
        for j in range(D // width):
            cols = pl.ds(j * width, width)
            x_v[rows, cols] = (x_v[rows, cols].astype(F32) + dot(act_v[rows, :], down_v[:, cols])).astype(BF16)
            if out_copy is not None:
                out_copy(j).start()

    def k_copy(s, piece, slot, dst):
        return pltpu.make_async_remote_copy(src_ref=kv_v.at[s, piece], dst_ref=kv_v.at[s, piece], send_sem=k_ssem.at[s, slot], recv_sem=k_rsem.at[s, piece],
                                            device_id={'seq': dst}, device_id_type=pl.DeviceIdType.MESH)

    def v_copy(s, piece, slot, dst):
        return pltpu.make_async_remote_copy(src_ref=vt_v.at[s, piece], dst_ref=vt_v.at[s, piece], send_sem=v_ssem.at[s, slot], recv_sem=v_rsem.at[s, piece],
                                            device_id={'seq': dst}, device_id_type=pl.DeviceIdType.MESH)

    def kv_send(s, piece, slot, dst):
        k_copy(s, piece, slot, dst).start()
        v_copy(s, piece, slot, dst).start()

    def kv_wait(s, piece):
        k_copy(s, piece, 0, 0).wait_recv()
        v_copy(s, piece, 0, 0).wait_recv()

    def kv_sent(s, piece, slot, dst):
        k_copy(s, piece, slot, dst).wait_send()
        v_copy(s, piece, slot, dst).wait_send()

    def rope(first, second):
        cos = cos_v[...]
        sin = sin_v[...]
        return first * cos - second * sin, second * cos + first * sin

    def qkv(s):
        rows = pl.ds(s * TOK, TOK)
        norm_rows(s * TOK, TOK)
        kv_t = dot_t(wqkv_v[QH * HD:, :], u_v[rows, :])
        parts = []
        for g in range(2):
            parts.extend(rope(kv_t[g * HD:g * HD + 32], kv_t[g * HD + 32:g * HD + HD]))
        kv_v[s, me] = jnp.concatenate(parts, axis=0).T.astype(BF16)
        vt_v[s, me] = kv_t[2 * HD:].astype(BF16)
        q_t = dot_t(wqkv_v[:QH * HD, :], u_v[rows, :])
        for h in range(QH):
            top = (h // 4) * HD
            lo, hi = rope(q_t[h * HD:h * HD + 32], q_t[h * HD + 32:h * HD + HD])
            qz_v[h, top:top + 32, :] = (lo * 0.125).astype(BF16)
            qz_v[h, top + 32:top + HD, :] = (hi * 0.125).astype(BF16)

        @pl.when(me == 0)
        def _():
            kv_send(s, 0, 0, 1)
            kv_send(s, 0, 1, 2)

        @pl.when(me == 1)
        def _():
            kv_send(s, 1, 0, 3)

        @pl.when(me == 2)
        def _():
            kv_send(s, 2, 0, 3)
            kv_wait(s, 0)
            kv_send(s, 0, 1, 3)

        @pl.when(me == 3)
        def _():
            kv_wait(s, 1)
            kv_send(s, 1, 0, 2)

    def attend(s, piece, first):
        causal = iota((TOK, TOK), 0) <= iota((TOK, TOK), 1)

        def score(h):
            sc_v[h] = dot(kv_v[s, piece], qz_v[h])

        def soft(h):
            sc = sc_v[h]
            if first:
                sc = jnp.where(causal, sc, -jnp.inf)
                top = jnp.max(sc, axis=0, keepdims=True)
                prob = jnp.exp(sc - top)
                l_v[h] = jnp.sum(prob, axis=0, keepdims=True)
                fix = None
            else:
                old = m_v[h]
                top = jnp.maximum(old, jnp.max(sc, axis=0, keepdims=True))
                fix = jnp.exp(old - top)
                prob = jnp.exp(sc - top)
                l_v[h] = l_v[h] * fix + jnp.sum(prob, axis=0, keepdims=True)
            m_v[h] = top
            pr_v[h] = prob.astype(BF16)
            return fix

        def mix(h, fix):
            g = h // 4
            out = dot(vt_v[s, piece, g * HD:(g + 1) * HD, :], pr_v[h])
            acc_v[h] = out if first else acc_v[h] * fix + out

        score(0)
        score(1)
        fixes = {}
        for h in range(QH):
            if h + 2 < QH:
                score(h + 2)
            fixes[h] = soft(h)
            if h >= 1:
                mix(h - 1, fixes[h - 1])
        mix(QH - 1, fixes[QH - 1])

    def attention(s):
        attend(s, me, True)

        def older(piece, carry):
            early = ((me == 2) & (piece == 0)) | ((me == 3) & (piece == 1))

            @pl.when(jnp.logical_not(early))
            def _():
                kv_wait(s, piece)
            attend(s, piece, False)
            return carry
        lax.fori_loop(0, me, older, 0)
        rows = pl.ds(s * TOK, TOK)
        for pair in range(QH // 2):
            top = acc_v[2 * pair] / l_v[2 * pair]
            bot = acc_v[2 * pair + 1] / l_v[2 * pair + 1]
            att_v[:, pair * 128:(pair + 1) * 128] = jnp.concatenate([top, bot], axis=0).T.astype(BF16)
        for j in range(D // 512):
            cols = pl.ds(j * 512, 512)
            x_v[rows, cols] = (x_v[rows, cols].astype(F32) + dot(att_v[...], wo_v[:, cols])).astype(BF16)

    copies['wout'].wait()
    ssd_finish(0)
    norm_rows(0, TOK)
    copies['up'].wait()
    mlp_up(0, TOK, 512, 2)
    copies['down'].wait()
    mlp_down(0, TOK, 512)
    for name in ('wq', 'wkv', 'wo', 'cos', 'sin'):
        copies[name].wait()
    qkv(0)
    attention(0)
    ssd_finish(1)
    norm_rows(TOK, TOK)
    mlp_up(TOK, TOK, 512, 2)
    load('up', up2_h, up_v, 7)
    mlp_down(TOK, TOK, 512)
    load('down', down2_h, down_v, 8)
    qkv(1)
    attention(1)
    norm_rows(0, ROWS)
    copies['up'].wait()
    mlp_up(0, ROWS, 256, 2)
    copies['down'].wait()

    def out_copy(j):
        cols = pl.ds(j * 256, 256)
        return pltpu.make_async_copy(x_v.at[:, cols], out_h.at[:, cols], osem.at[j])
    mlp_down(0, ROWS, 256, out_copy)

    @pl.when(me < 3)
    def _():
        for s in range(NSEQ):
            for ch in range(NCH):
                st_copy(s, ch, 0).wait_send()
    for s in range(NSEQ):
        kv_sent(s, 0, 0, 0)

        @pl.when((me == 0) | (me == 2))
        def _():
            kv_sent(s, 0, 1, 0)
    for j in range(D // 256):
        out_copy(j).wait()


def rope_tables(seq_len):
    inv = (np.float32(ROPE_BASE) ** (-(np.arange(32, dtype=np.float32) * np.float32(2.0) / np.float32(HD)))).astype(np.float32)
    ang = (inv[:, None] * np.arange(seq_len, dtype=np.float32)[None, :]).astype(np.float32).astype(np.float64)
    return np.cos(ang).astype(np.float32), np.sin(ang).astype(np.float32)


def solution(mesh):
    n_dev = mesh.shape['seq']
    cos_t, sin_t = rope_tables(n_dev * TOK)
    any_spec = pl.BlockSpec(memory_space=pl.ANY)
    vm_spec = pl.BlockSpec(memory_space=pltpu.VMEM)
    vm = pltpu.VMEM
    call = pl.pallas_call(
        kernel,
        out_shape=jax.ShapeDtypeStruct((ROWS, D), BF16),
        in_specs=[any_spec, any_spec, vm_spec, vm_spec, vm_spec] + [any_spec] * 10,
        out_specs=any_spec,
        scratch_shapes=[
            vm((ROWS, D), BF16), vm((ROWS, D), BF16), vm((INNER, D), BF16), vm((INNER, D), BF16), vm((2 * NST + HEADS, D), BF16),
            vm((INNER, D), BF16), vm((D, 2 * FF), BF16), vm((FF, D), BF16), vm((QH * HD + 256, D), BF16), vm((QH * HD, D), BF16),
            vm((32, TOK), F32), vm((32, TOK), F32),
            vm((ROWS, INNER), BF16), vm((ROWS, INNER), BF16), vm((ROWS, NST), BF16), vm((ROWS, NST), BF16),
            vm((ROWS, 128), BF16), vm((ROWS, 128), BF16), vm((128, INNER), BF16), vm((GW, GW), BF16),
            vm((ROWS, INNER), F32), vm((ROWS, INNER), F32), vm((ROWS, INNER), F32), vm((NSEQ * NBLK * 8, INNER), F32), vm((8, INNER), F32),
            vm((NSEQ * NBLK, NCH, NST, CHW), F32), vm((NSEQ, NCH, NST, CHW), F32), vm((NSEQ, NCH, NST, CHW), F32), vm((ROWS, FF), BF16),
            vm((QH, 2 * HD, TOK), BF16), vm((NSEQ, 4, TOK, 128), BF16), vm((NSEQ, 4, 128, TOK), BF16),
            vm((QH, 1, TOK), F32), vm((QH, 1, TOK), F32), vm((QH, HD, TOK), F32), vm((TOK, QH * HD), BF16),
            vm((QH, TOK, TOK), F32), vm((QH, TOK, TOK), BF16),
            pltpu.SemaphoreType.DMA((14,)), pltpu.SemaphoreType.DMA((4,)), pltpu.SemaphoreType.DMA((NSEQ, NCH)), pltpu.SemaphoreType.DMA((NSEQ, NCH)),
            pltpu.SemaphoreType.DMA((NSEQ, 2)), pltpu.SemaphoreType.DMA((NSEQ, 4)), pltpu.SemaphoreType.DMA((NSEQ, 2)), pltpu.SemaphoreType.DMA((NSEQ, 4)),
        ],
        compiler_params=pltpu.CompilerParams(collective_id=0, has_side_effects=True, vmem_limit_bytes=67_000_000),
        name='layer_stack',
    )

    def local_fn(x_loc, w_in, dt_bias, a_neg, d_skip, w_out, w_up1, w_down1, w_q, w_kv, w_o, w_up2, w_down2):
        w_q_t = w_q.transpose(1, 2, 0).reshape(QH * HD, D)
        w_kv_t = w_kv.transpose(1, 2, 3, 0).reshape(256, D)
        out = call(x_loc.reshape(ROWS, D), w_in.T, dt_bias.reshape(1, HEADS), a_neg.reshape(1, HEADS), d_skip.reshape(1, HEADS), w_out, w_up1, w_down1,
                   w_q_t, w_kv_t, w_o.reshape(QH * HD, D), w_up2, w_down2, jnp.asarray(cos_t), jnp.asarray(sin_t))
        return out.reshape(x_loc.shape)

    seq_spec = P('data', 'seq', None)
    return jax.shard_map(local_fn, mesh=mesh, in_specs=(seq_spec,) + (P(),) * 12, out_specs=seq_spec, check_vma=False)
```

```python
import functools
import jax
import jax.numpy as jnp
import numpy as np
from jax import lax
from jax.experimental import pallas as pl
from jax.experimental.pallas import tpu as pltpu
from jax.sharding import PartitionSpec as P

F32 = jnp.float32
BF16 = jnp.bfloat16
BLK = 64
EPS = 1e-6
ROPE_BASE = 10000.0
NSEQ = 2
TOK = 256
NBLK = TOK // BLK
ROWS = NSEQ * TOK
D = 1024
INNER = 1536
HEADS = 24
NST = 128
FF = 2048
NCH = 6
CHW = INNER // NCH
GW = 256
HD = 64
QH = 8


def dot(a, b):
    return jnp.dot(a, b, preferred_element_type=F32)


def dot_t(a, b):
    return lax.dot_general(a, b, (((1,), (1,)), ((), ())), preferred_element_type=F32)


def hdot(a, b):
    return jnp.dot(a, b, preferred_element_type=F32, precision=lax.Precision.HIGHEST)


def iota(shape, dim):
    return lax.broadcasted_iota(jnp.int32, shape, dim)


def split3(v, lane):
    hi = v.astype(BF16)
    rest = v - hi.astype(F32)
    mid = rest.astype(BF16)
    low = rest - mid.astype(F32)
    return jnp.where(lane < 32, hi.astype(F32), jnp.where(lane < 64, mid.astype(F32), low)).astype(BF16)


def silu(v):
    return v * jax.nn.sigmoid(v)


def kernel(x_h, win_h, bias_r, aneg_r, dskip_r, wout_h, up1_h, down1_h, wq_h, wkv_h, wo_h, up2_h, down2_h, cos_h, sin_h, out_h,
           x_v, u_v, wx_v, wz_v, wt_v, wout_v, up_v, down_v, wqkv_v, wo_v, cos_v, sin_v,
           xs_v, z_v, b_v, c_v, csp_v, dsp_v, e4_v, bd_v, y_v, ec_v, de_v, el_v, dsk_v, bs_v, e_v, hin_v, act_v,
           qz_v, kv_v, vt_v, m_v, l_v, acc_v, att_v, sc_v, pr_v, sc4_v, bt_v,
           lsem, osem, st_ssem, st_rsem, k_ssem, k_rsem, v_ssem, v_rsem):
    me = lax.axis_index('seq')
    copies = {}

    def load(name, src, dst, idx):
        copies[name] = pltpu.make_async_copy(src, dst, lsem.at[idx])
        copies[name].start()

    load('x', x_h, x_v, 0)
    load('wt', win_h.at[pl.ds(2 * INNER, 2 * NST + HEADS), :], wt_v, 1)
    load('wx0', win_h.at[pl.ds(0, CHW), :], wx_v.at[pl.ds(0, CHW), :], 2)
    load('wx1', win_h.at[pl.ds(CHW, INNER - CHW), :], wx_v.at[pl.ds(CHW, INNER - CHW), :], 3)
    load('wz', win_h.at[pl.ds(INNER, INNER), :], wz_v, 5)

    barrier = pltpu.get_barrier_semaphore()
    for off in (1, 2, 3):
        pl.semaphore_signal(barrier, inc=1, device_id={'seq': lax.rem(me + off, 4)}, device_id_type=pl.DeviceIdType.MESH)

    spread = ((iota((HEADS, 128), 1) & 31) == iota((HEADS, 128), 0)) & (iota((HEADS, 128), 1) < 96)
    spread = spread.astype(F32)
    lane8 = iota((8, 128), 1)
    bias3 = hdot(jnp.broadcast_to(bias_r[...], (8, HEADS)), spread)[0:1]
    aneg3 = hdot(jnp.broadcast_to(aneg_r[...], (8, HEADS)), spread)[0:1]
    dsk3 = split3(hdot(jnp.broadcast_to(dskip_r[...], (8, HEADS)), spread), lane8)
    for g in range(INNER // GW):
        cols = pl.ds(g * GW, GW)
        head = (iota((128, GW), 1) + g * GW) >> 6
        row = iota((128, GW), 0)
        e4_v[:, cols] = (((row & 31) == head) & (row < 96)).astype(F32).astype(BF16)
        dsk_v[:, cols] = dot(dsk3, e4_v[:, cols])
    bd_v[...] = ((iota((GW, GW), 0) >> 6) == (iota((GW, GW), 1) >> 6)).astype(F32).astype(BF16)
    for h in range(QH):
        qz_v[h] = jnp.zeros((2 * HD, TOK), BF16)

    @pl.when(me == 0)
    def _():
        for s in range(NSEQ):
            for ch in range(NCH):
                hin_v[s, ch] = jnp.zeros((NST, CHW), F32)

    def norm_rows(start, count):
        def body(step, carry):
            rows = pl.ds(pl.multiple_of(start + step * 128, 128), 128)
            vals = x_v[rows, :].astype(F32)
            scale = lax.rsqrt(jnp.mean(vals * vals, axis=-1, keepdims=True) + EPS)
            u_v[rows, :] = (x_v[rows, :].astype(F32) * scale).astype(BF16)
            return carry
        lax.fori_loop(0, count // 128, body, 0, unroll=2)

    copies['x'].wait()
    norm_rows(0, ROWS)
    copies['wt'].wait()
    copies['wx0'].wait()

    spread_bf = spread.astype(BF16)
    tri = (iota((TOK, TOK), 0) >= iota((TOK, TOK), 1)) & ((iota((TOK, TOK), 0) >> 6) == (iota((TOK, TOK), 1) >> 6))
    tri = tri.astype(F32).astype(BF16)
    lane = iota((TOK, 128), 1)

    def decay_sums(s):
        rows = pl.ds(s * TOK, TOK)
        r_bf = dot_t(u_v[rows, :], wt_v[2 * NST:, :]).astype(BF16)
        pre = dot(r_bf, spread_bf) + bias3
        dt = jnp.maximum(pre, 0.0) + jnp.log1p(jnp.exp(-jnp.abs(pre)))
        part = dot(tri, split3(dt * aneg3, lane))
        cum = (part + pltpu.roll(part, 96, 1)) + pltpu.roll(part, 64, 1)
        cum = jnp.where(lane < 32, cum, jnp.where(lane < 64, pltpu.roll(cum, 32, 1), pltpu.roll(cum, 64, 1)))
        csp_v[rows, :] = split3(cum, lane)
        dsp_v[rows, :] = split3(dt, lane)

    def block_scores(s):
        rows = pl.ds(s * TOK, TOK)
        bc = dot_t(u_v[rows, :], wt_v[:2 * NST, :])
        b_v[rows, :] = bc[:, :NST].astype(BF16)
        c_v[rows, :] = bc[:, NST:].astype(BF16)
        for b in range(NBLK):
            i = s * NBLK + b
            blk = pl.ds(i * BLK, BLK)
            bb = b_v[blk, :]
            sc4_v[blk, :] = dot_t(c_v[blk, :], jnp.concatenate([bb] * 4, axis=0))
            bt_v[i] = bb.astype(F32).T.astype(BF16)

    decay_sums(0)
    decay_sums(1)
    block_scores(0)

    def proj_x(ch):
        cols = pl.ds(ch * CHW, CHW)
        xs_v[:, cols] = dot_t(u_v[...], wx_v[cols, :]).astype(BF16)

    def head_spread(ch):
        cols = pl.ds(ch * CHW, CHW)
        ec_v[:, cols] = dot(csp_v[...], e4_v[:, cols])
        de_v[:, cols] = dot(dsp_v[...], e4_v[:, cols])

    t_idx = iota((BLK, GW), 0)
    s_idx = iota((BLK, GW), 1) & (BLK - 1)

    def ssd_blocks(s, ch):
        for b in range(NBLK):
            i = s * NBLK + b
            rows = pl.ds(i * BLK, BLK)
            for half in range(CHW // GW):
                off = half * GW
                cols = pl.ds(ch * CHW + off, GW)
                ce = ec_v[rows, cols]
                de = de_v[rows, cols]
                crow = jnp.sum(jnp.where(t_idx == s_idx, ce, 0.0), axis=0, keepdims=True)
                drow = jnp.sum(jnp.where(t_idx == s_idx, de, 0.0), axis=0, keepdims=True)
                decay = jnp.exp(jnp.where(t_idx >= s_idx, ce - crow, -jnp.inf))
                mix = (sc4_v[rows, :] * decay * drow).astype(BF16)
                xg = xs_v[rows, cols]
                xw = xg.astype(F32)
                xbd = jnp.concatenate([xg] * 4, axis=0) * bd_v[...]
                y_v[rows, cols] = dot(mix, xbd) + dsk_v[0:1, cols] * xw
                last = ce[BLK - 1:BLK, :]
                state = dot(bt_v[i], (xw * (jnp.exp(last - ce) * de)).astype(BF16))
                bs_v[i, ch, :, off:off + GW] = state
                ec_v[rows, cols] = jnp.exp(ce)
                el_v[i * 8:i * 8 + 8, cols] = jnp.broadcast_to(jnp.exp(last), (8, GW))
        cols = pl.ds(ch * CHW, CHW)
        end = bs_v[s * NBLK, ch]
        for b in range(1, NBLK):
            i = s * NBLK + b
            end = el_v[i * 8:i * 8 + 1, cols] * end + bs_v[i, ch]
        e_v[s, ch] = end

    def st_copy(s, ch, dst):
        return pltpu.make_async_remote_copy(src_ref=e_v.at[s, ch], dst_ref=hin_v.at[s, ch], send_sem=st_ssem.at[s, ch], recv_sem=st_rsem.at[s, ch],
                                            device_id={'seq': dst}, device_id_type=pl.DeviceIdType.MESH)

    def chain(s, ch, dst):
        cols = pl.ds(ch * CHW, CHW)
        total = el_v[(s * NBLK) * 8:(s * NBLK) * 8 + 1, cols]
        for b in range(1, NBLK):
            total = total * el_v[(s * NBLK + b) * 8:(s * NBLK + b) * 8 + 1, cols]
        e_v[s, ch] = total * hin_v[s, ch] + e_v[s, ch]
        st_copy(s, ch, dst).start()

    def first_send(s, ch):
        @pl.when(me == 0)
        def _():
            st_copy(s, ch, 1).start()

    def relay(s, *chunks):
        @pl.when(me == 1)
        def _():
            for ch in chunks:
                st_copy(s, ch, 2).wait_recv()
                chain(s, ch, 2)

    def proj_z(ch):
        cols = pl.ds(ch * CHW, CHW)
        z_v[:, cols] = dot_t(u_v[...], wz_v[cols, :]).astype(BF16)

    proj_x(0)
    head_spread(0)
    ssd_blocks(0, 0)
    @pl.when(me == 0)
    def _():
        pl.semaphore_wait(barrier, 3)
        st_copy(0, 0, 1).start()

    @pl.when(me != 0)
    def _():
        pl.semaphore_wait(barrier, 3)

    copies['wx1'].wait()
    load('wout', wout_h, wout_v, 6)
    load('up', up1_h, up_v, 7)
    proj_x(1)
    head_spread(1)
    block_scores(1)
    for ch in range(1, NCH):
        if ch + 1 < NCH:
            proj_x(ch + 1)
            head_spread(ch + 1)
        ssd_blocks(0, ch)
        first_send(0, ch)
        relay(0, ch - 1)
    load('down', down1_h, down_v, 8)
    load('wq', wq_h, wqkv_v.at[pl.ds(0, QH * HD), :], 9)
    load('wkv', wkv_h, wqkv_v.at[pl.ds(QH * HD, 256), :], 10)
    load('wo', wo_h, wo_v, 11)
    tab = pl.ds(pl.multiple_of(me * TOK, TOK), TOK)
    load('cos', cos_h.at[:, tab], cos_v, 12)
    load('sin', sin_h.at[:, tab], sin_v, 13)
    copies['wz'].wait()
    for ch in range(NCH):
        proj_z(ch)
        ssd_blocks(1, ch)
        first_send(1, ch)
        if ch == 0:
            relay(0, NCH - 1)
        elif ch >= 2:
            relay(1, ch - 2)
    relay(1, NCH - 2, NCH - 1)

    def ssd_finish(s):
        for group in (range(NCH // 2), range(NCH // 2, NCH)):
            @pl.when(me == 2)
            def _(group=group):
                for ch in group:
                    st_copy(s, ch, 3).wait_recv()
                    chain(s, ch, 3)

            @pl.when(me == 3)
            def _(group=group):
                for ch in group:
                    st_copy(s, ch, 3).wait_recv()

            for ch in group:
                cols = pl.ds(ch * CHW, CHW)
                held = hin_v[s, ch]
                for b in range(NBLK):
                    i = s * NBLK + b
                    rows = pl.ds(i * BLK, BLK)
                    y_v[rows, cols] = y_v[rows, cols] + ec_v[rows, cols] * dot(c_v[rows, :], held.astype(BF16))
                    if b < NBLK - 1:
                        held = el_v[i * 8:i * 8 + 1, cols] * held + bs_v[i, ch]

        def gate(b, carry):
            rows = pl.ds(pl.multiple_of(s * TOK + b * BLK, BLK), BLK)
            ssq = jnp.zeros((BLK, 1), F32)
            for ch in range(NCH):
                yv = y_v[rows, ch * CHW:(ch + 1) * CHW]
                ssq = ssq + jnp.sum(yv * yv, axis=-1, keepdims=True)
            scale = lax.rsqrt(ssq * (1.0 / INNER) + EPS)
            for ch in range(NCH):
                cols = pl.ds(ch * CHW, CHW)
                xs_v[rows, cols] = (y_v[rows, cols] * scale * silu(z_v[rows, cols].astype(F32))).astype(BF16)
            return carry
        lax.fori_loop(0, NBLK, gate, 0, unroll=2)

        rows = pl.ds(s * TOK, TOK)
        for j in range(D // 512):
            cols = pl.ds(j * 512, 512)
            x_v[rows, cols] = (x_v[rows, cols].astype(F32) + dot(xs_v[rows, :], wout_v[:, cols])).astype(BF16)

    def mlp_up(start, count):
        rows = pl.ds(start, count)
        for j in range(FF // 256):
            gate = dot(u_v[rows, :], up_v[:, j * 256:(j + 1) * 256])
            up = dot(u_v[rows, :], up_v[:, FF + j * 256:FF + (j + 1) * 256])
            act_v[rows, j * 256:(j + 1) * 256] = (silu(gate) * up).astype(BF16)

    def mlp_down(start, count, width, out_copy=None):
        rows = pl.ds(start, count)
        for j in range(D // width):
            cols = pl.ds(j * width, width)
            x_v[rows, cols] = (x_v[rows, cols].astype(F32) + dot(act_v[rows, :], down_v[:, cols])).astype(BF16)
            if out_copy is not None:
                out_copy(j).start()

    def k_copy(s, piece, slot, dst):
        return pltpu.make_async_remote_copy(src_ref=kv_v.at[s, piece], dst_ref=kv_v.at[s, piece], send_sem=k_ssem.at[s, slot], recv_sem=k_rsem.at[s, piece],
                                            device_id={'seq': dst}, device_id_type=pl.DeviceIdType.MESH)

    def v_copy(s, piece, slot, dst):
        return pltpu.make_async_remote_copy(src_ref=vt_v.at[s, piece], dst_ref=vt_v.at[s, piece], send_sem=v_ssem.at[s, slot], recv_sem=v_rsem.at[s, piece],
                                            device_id={'seq': dst}, device_id_type=pl.DeviceIdType.MESH)

    def kv_send(s, piece, slot, dst):
        k_copy(s, piece, slot, dst).start()
        v_copy(s, piece, slot, dst).start()

    def kv_wait(s, piece):
        k_copy(s, piece, 0, 0).wait_recv()
        v_copy(s, piece, 0, 0).wait_recv()

    def kv_sent(s, piece, slot, dst):
        k_copy(s, piece, slot, dst).wait_send()
        v_copy(s, piece, slot, dst).wait_send()

    def rope(first, second):
        cos = cos_v[...]
        sin = sin_v[...]
        return first * cos - second * sin, second * cos + first * sin

    def qkv(s):
        rows = pl.ds(s * TOK, TOK)
        norm_rows(s * TOK, TOK)
        kv_t = dot_t(wqkv_v[QH * HD:, :], u_v[rows, :])
        parts = []
        for g in range(2):
            parts.extend(rope(kv_t[g * HD:g * HD + 32], kv_t[g * HD + 32:g * HD + HD]))
        kv_v[s, me] = jnp.concatenate(parts, axis=0).T.astype(BF16)
        vt_v[s, me] = kv_t[2 * HD:].astype(BF16)
        q_t = dot_t(wqkv_v[:QH * HD, :], u_v[rows, :])
        for h in range(QH):
            top = (h // 4) * HD
            lo, hi = rope(q_t[h * HD:h * HD + 32], q_t[h * HD + 32:h * HD + HD])
            qz_v[h, top:top + 32, :] = (lo * 0.125).astype(BF16)
            qz_v[h, top + 32:top + HD, :] = (hi * 0.125).astype(BF16)

        @pl.when(me == 0)
        def _():
            kv_send(s, 0, 0, 1)
            kv_send(s, 0, 1, 2)

        @pl.when(me == 1)
        def _():
            kv_send(s, 1, 0, 3)

        @pl.when(me == 2)
        def _():
            kv_send(s, 2, 0, 3)
            kv_wait(s, 0)
            kv_send(s, 0, 1, 3)

        @pl.when(me == 3)
        def _():
            kv_wait(s, 1)
            kv_send(s, 1, 0, 2)

    def attend(s, piece, first):
        causal = iota((TOK, TOK), 0) <= iota((TOK, TOK), 1)

        def score(h):
            sc_v[h] = dot(kv_v[s, piece], qz_v[h])

        def soft(h):
            pieces = range(TOK // 64)

            def load_scores(r):
                sc = sc_v[h, r * 64:(r + 1) * 64, :]
                return jnp.where(causal[r * 64:(r + 1) * 64], sc, -jnp.inf) if first else sc

            top = jnp.concatenate([jnp.max(load_scores(r).reshape(8, 8, TOK), axis=0) for r in pieces], axis=0)
            top = jnp.max(top, axis=0, keepdims=True)
            fix = None
            if not first:
                old = m_v[h]
                top = jnp.maximum(old, top)
                fix = jnp.exp(old - top)
            total = jnp.zeros((8, TOK), F32)
            for r in pieces:
                prob = jnp.exp(load_scores(r) - top)
                total = total + jnp.sum(prob.reshape(8, 8, TOK), axis=0)
                pr_v[h, r * 64:(r + 1) * 64, :] = prob.astype(BF16)
            total = jnp.sum(total, axis=0, keepdims=True)
            l_v[h] = total if first else l_v[h] * fix + total
            m_v[h] = top
            return fix

        def mix(h, fix):
            g = h // 4
            out = dot(vt_v[s, piece, g * HD:(g + 1) * HD, :], pr_v[h])
            acc_v[h] = out if first else acc_v[h] * fix + out

        score(0)
        score(1)
        fixes = {}
        for h in range(QH):
            if h + 2 < QH:
                score(h + 2)
            fixes[h] = soft(h)
            if h >= 1:
                mix(h - 1, fixes[h - 1])
        mix(QH - 1, fixes[QH - 1])

    def attention(s):
        attend(s, me, True)

        def older(piece, carry):
            early = ((me == 2) & (piece == 0)) | ((me == 3) & (piece == 1))

            @pl.when(jnp.logical_not(early))
            def _():
                kv_wait(s, piece)
            attend(s, piece, False)
            return carry
        lax.fori_loop(0, me, older, 0)
        rows = pl.ds(s * TOK, TOK)
        for pair in range(QH // 2):
            top = acc_v[2 * pair] / l_v[2 * pair]
            bot = acc_v[2 * pair + 1] / l_v[2 * pair + 1]
            att_v[:, pair * 128:(pair + 1) * 128] = jnp.concatenate([top, bot], axis=0).T.astype(BF16)
        for j in range(D // 512):
            cols = pl.ds(j * 512, 512)
            x_v[rows, cols] = (x_v[rows, cols].astype(F32) + dot(att_v[...], wo_v[:, cols])).astype(BF16)

    copies['wout'].wait()
    ssd_finish(0)
    norm_rows(0, TOK)
    copies['up'].wait()
    mlp_up(0, TOK)
    copies['down'].wait()
    mlp_down(0, TOK, 512)
    for name in ('wq', 'wkv', 'wo', 'cos', 'sin'):
        copies[name].wait()
    qkv(0)
    attention(0)
    ssd_finish(1)
    norm_rows(TOK, TOK)
    mlp_up(TOK, TOK)
    load('up', up2_h, up_v, 7)
    mlp_down(TOK, TOK, 512)
    load('down', down2_h, down_v, 8)
    qkv(1)
    attention(1)
    norm_rows(0, ROWS)
    copies['up'].wait()
    mlp_up(0, ROWS)
    copies['down'].wait()

    def out_copy(j):
        cols = pl.ds(j * 256, 256)
        return pltpu.make_async_copy(x_v.at[:, cols], out_h.at[:, cols], osem.at[j])
    mlp_down(0, ROWS, 256, out_copy)

    @pl.when(me < 3)
    def _():
        for s in range(NSEQ):
            for ch in range(NCH):
                st_copy(s, ch, 0).wait_send()
    for s in range(NSEQ):
        kv_sent(s, 0, 0, 0)

        @pl.when((me == 0) | (me == 2))
        def _():
            kv_sent(s, 0, 1, 0)
    for j in range(D // 256):
        out_copy(j).wait()


def rope_tables(seq_len):
    inv = (np.float32(ROPE_BASE) ** (-(np.arange(32, dtype=np.float32) * np.float32(2.0) / np.float32(HD)))).astype(np.float32)
    ang = (inv[:, None] * np.arange(seq_len, dtype=np.float32)[None, :]).astype(np.float32).astype(np.float64)
    return np.cos(ang).astype(np.float32), np.sin(ang).astype(np.float32)


def solution(mesh):
    n_dev = mesh.shape['seq']
    cos_t, sin_t = rope_tables(n_dev * TOK)
    any_spec = pl.BlockSpec(memory_space=pl.ANY)
    vm_spec = pl.BlockSpec(memory_space=pltpu.VMEM)
    vm = pltpu.VMEM
    call = pl.pallas_call(
        kernel,
        out_shape=jax.ShapeDtypeStruct((ROWS, D), BF16),
        in_specs=[any_spec, any_spec, vm_spec, vm_spec, vm_spec] + [any_spec] * 10,
        out_specs=any_spec,
        scratch_shapes=[
            vm((ROWS, D), BF16), vm((ROWS, D), BF16), vm((INNER, D), BF16), vm((INNER, D), BF16), vm((2 * NST + HEADS, D), BF16),
            vm((INNER, D), BF16), vm((D, 2 * FF), BF16), vm((FF, D), BF16), vm((QH * HD + 256, D), BF16), vm((QH * HD, D), BF16),
            vm((32, TOK), F32), vm((32, TOK), F32),
            vm((ROWS, INNER), BF16), vm((ROWS, INNER), BF16), vm((ROWS, NST), BF16), vm((ROWS, NST), BF16),
            vm((ROWS, 128), BF16), vm((ROWS, 128), BF16), vm((128, INNER), BF16), vm((GW, GW), BF16),
            vm((ROWS, INNER), F32), vm((ROWS, INNER), F32), vm((ROWS, INNER), F32), vm((NSEQ * NBLK * 8, INNER), F32), vm((8, INNER), F32),
            vm((NSEQ * NBLK, NCH, NST, CHW), F32), vm((NSEQ, NCH, NST, CHW), F32), vm((NSEQ, NCH, NST, CHW), F32), vm((ROWS, FF), BF16),
            vm((QH, 2 * HD, TOK), BF16), vm((NSEQ, 4, TOK, 128), BF16), vm((NSEQ, 4, 128, TOK), BF16),
            vm((QH, 1, TOK), F32), vm((QH, 1, TOK), F32), vm((QH, HD, TOK), F32), vm((TOK, QH * HD), BF16),
            vm((QH, TOK, TOK), F32), vm((QH, TOK, TOK), BF16), vm((ROWS, GW), F32), vm((NSEQ * NBLK, NST, BLK), BF16),
            pltpu.SemaphoreType.DMA((14,)), pltpu.SemaphoreType.DMA((4,)), pltpu.SemaphoreType.DMA((NSEQ, NCH)), pltpu.SemaphoreType.DMA((NSEQ, NCH)),
            pltpu.SemaphoreType.DMA((NSEQ, 2)), pltpu.SemaphoreType.DMA((NSEQ, 4)), pltpu.SemaphoreType.DMA((NSEQ, 2)), pltpu.SemaphoreType.DMA((NSEQ, 4)),
        ],
        compiler_params=pltpu.CompilerParams(collective_id=0, has_side_effects=True, vmem_limit_bytes=67_000_000),
        name='layer_stack',
    )

    def local_fn(x_loc, w_in, dt_bias, a_neg, d_skip, w_out, w_up1, w_down1, w_q, w_kv, w_o, w_up2, w_down2):
        w_q_t = w_q.transpose(1, 2, 0).reshape(QH * HD, D)
        w_kv_t = w_kv.transpose(1, 2, 3, 0).reshape(256, D)
        out = call(x_loc.reshape(ROWS, D), w_in.T, dt_bias.reshape(1, HEADS), a_neg.reshape(1, HEADS), d_skip.reshape(1, HEADS), w_out, w_up1, w_down1,
                   w_q_t, w_kv_t, w_o.reshape(QH * HD, D), w_up2, w_down2, jnp.asarray(cos_t), jnp.asarray(sin_t))
        return out.reshape(x_loc.shape)

    seq_spec = P('data', 'seq', None)
    return jax.shard_map(local_fn, mesh=mesh, in_specs=(seq_spec,) + (P(),) * 12, out_specs=seq_spec, check_vma=False)
```

```python
import functools
import jax
import jax.numpy as jnp
import numpy as np
from jax import lax
from jax.experimental import pallas as pl
from jax.experimental.pallas import tpu as pltpu
from jax.sharding import PartitionSpec as P

F32 = jnp.float32
BF16 = jnp.bfloat16
BLK = 64
EPS = 1e-6
ROPE_BASE = 10000.0
NSEQ = 2
TOK = 256
NBLK = TOK // BLK
ROWS = NSEQ * TOK
D = 1024
INNER = 1536
HEADS = 24
NST = 128
FF = 2048
NCH = 6
CHW = INNER // NCH
GW = 256
HD = 64
QH = 8


def dot(a, b):
    return jnp.dot(a, b, preferred_element_type=F32)


def dot_t(a, b):
    return lax.dot_general(a, b, (((1,), (1,)), ((), ())), preferred_element_type=F32)


def hdot(a, b):
    return jnp.dot(a, b, preferred_element_type=F32, precision=lax.Precision.HIGHEST)


def iota(shape, dim):
    return lax.broadcasted_iota(jnp.int32, shape, dim)


def split3(v, lane):
    hi = v.astype(BF16)
    rest = v - hi.astype(F32)
    mid = rest.astype(BF16)
    low = rest - mid.astype(F32)
    return jnp.where(lane < 32, hi.astype(F32), jnp.where(lane < 64, mid.astype(F32), low)).astype(BF16)


def silu(v):
    return v * jax.nn.sigmoid(v)


def kernel(x_h, win_h, bias_r, aneg_r, dskip_r, wout_h, up1_h, down1_h, wq_h, wkv_h, wo_h, up2_h, down2_h, cos_h, sin_h, out_h,
           x_v, u_v, wx_v, wz_v, wt_v, wr_v, wout_v, up_v, down_v, wqkv_v, wo_v, cos_v, sin_v,
           xs_v, z_v, b_v, c_v, csp_v, dsp_v, e4_v, bd_v, y_v, ec_v, de_v, el_v, dsk_v, bs_v, e_v, hin_v, act_v,
           qz_v, kv_v, vt_v, m_v, l_v, acc_v, att_v, sc_v, pr_v, sc4_v, bt_v,
           lsem, osem, st_ssem, st_rsem, k_ssem, k_rsem, v_ssem, v_rsem):
    me = lax.axis_index('seq')
    copies = {}

    def load(name, src, dst, idx):
        copies[name] = pltpu.make_async_copy(src, dst, lsem.at[idx])
        copies[name].start()

    load('xa', x_h.at[pl.ds(0, TOK), :], x_v.at[pl.ds(0, TOK), :], 0)
    for k in range(3):
        load('wr%d' % k, win_h.at[pl.ds(2 * INNER + 2 * NST, HEADS), :], wr_v.at[pl.ds(32 * k, HEADS), :], 14 + k)
    load('wt', win_h.at[pl.ds(2 * INNER, 2 * NST), :], wt_v, 1)
    load('wx0', win_h.at[pl.ds(0, CHW), :], wx_v.at[pl.ds(0, CHW), :], 2)
    load('xb', x_h.at[pl.ds(TOK, TOK), :], x_v.at[pl.ds(TOK, TOK), :], 4)
    load('wx1', win_h.at[pl.ds(CHW, INNER - CHW), :], wx_v.at[pl.ds(CHW, INNER - CHW), :], 3)
    load('wz', win_h.at[pl.ds(INNER, INNER), :], wz_v, 5)

    barrier = pltpu.get_barrier_semaphore()
    for off in (1, 2, 3):
        pl.semaphore_signal(barrier, inc=1, device_id={'seq': lax.rem(me + off, 4)}, device_id_type=pl.DeviceIdType.MESH)

    spread = ((iota((HEADS, 128), 1) & 31) == iota((HEADS, 128), 0)) & (iota((HEADS, 128), 1) < 96)
    spread = spread.astype(F32)
    lane8 = iota((8, 128), 1)
    bias3 = hdot(jnp.broadcast_to(bias_r[...], (8, HEADS)), spread)[0:1]
    aneg3 = hdot(jnp.broadcast_to(aneg_r[...], (8, HEADS)), spread)[0:1]
    dsk3 = split3(hdot(jnp.broadcast_to(dskip_r[...], (8, HEADS)), spread), lane8)
    for g in range(INNER // GW):
        cols = pl.ds(g * GW, GW)
        head = (iota((128, GW), 1) + g * GW) >> 6
        row = iota((128, GW), 0)
        e4_v[:, cols] = (((row & 31) == head) & (row < 96)).astype(F32).astype(BF16)
        dsk_v[:, cols] = dot(dsk3, e4_v[:, cols])
    bd_v[...] = ((iota((GW, GW), 0) >> 6) == (iota((GW, GW), 1) >> 6)).astype(F32).astype(BF16)
    for lo, hi in ((24, 32), (56, 64), (88, 128)):
        wr_v[lo:hi, :] = jnp.zeros((hi - lo, D), BF16)
    for h in range(QH):
        qz_v[h] = jnp.zeros((2 * HD, TOK), BF16)

    @pl.when(me == 0)
    def _():
        for s in range(NSEQ):
            for ch in range(NCH):
                hin_v[s, ch] = jnp.zeros((NST, CHW), F32)

    def norm_rows(start, count):
        def body(step, carry):
            rows = pl.ds(pl.multiple_of(start + step * 128, 128), 128)
            vals = x_v[rows, :].astype(F32)
            scale = lax.rsqrt(jnp.mean(vals * vals, axis=-1, keepdims=True) + EPS)
            u_v[rows, :] = (x_v[rows, :].astype(F32) * scale).astype(BF16)
            return carry
        lax.fori_loop(0, count // 128, body, 0, unroll=2)

    copies['xa'].wait()
    norm_rows(0, TOK)
    for k in range(3):
        copies['wr%d' % k].wait()
    copies['wt'].wait()
    copies['wx0'].wait()

    tri = (iota((TOK, TOK), 0) >= iota((TOK, TOK), 1)) & ((iota((TOK, TOK), 0) >> 6) == (iota((TOK, TOK), 1) >> 6))
    tri = tri.astype(F32).astype(BF16)
    lane = iota((TOK, 128), 1)

    def decay_sums(s):
        rows = pl.ds(s * TOK, TOK)
        pre = dot_t(u_v[rows, :], wr_v[...]).astype(BF16).astype(F32) + bias3
        dt = jnp.maximum(pre, 0.0) + jnp.log1p(jnp.exp(-jnp.abs(pre)))
        part = dot(tri, split3(dt * aneg3, lane))
        cum = (part + pltpu.roll(part, 96, 1)) + pltpu.roll(part, 64, 1)
        cum = jnp.where(lane < 32, cum, jnp.where(lane < 64, pltpu.roll(cum, 32, 1), pltpu.roll(cum, 64, 1)))
        csp_v[rows, :] = split3(cum, lane)
        dsp_v[rows, :] = split3(dt, lane)

    def block_scores(s):
        rows = pl.ds(s * TOK, TOK)
        bc = dot_t(u_v[rows, :], wt_v[...])
        b_v[rows, :] = bc[:, :NST].astype(BF16)
        c_v[rows, :] = bc[:, NST:].astype(BF16)
        for b in range(NBLK):
            i = s * NBLK + b
            blk = pl.ds(i * BLK, BLK)
            bb = b_v[blk, :]
            sc4_v[blk, :] = dot_t(c_v[blk, :], jnp.concatenate([bb] * 4, axis=0))
            bt_v[i] = bb.astype(F32).T.astype(BF16)

    decay_sums(0)
    block_scores(0)

    def proj_x(ch, start=0, count=ROWS):
        cols = pl.ds(ch * CHW, CHW)
        rows = pl.ds(start, count)
        xs_v[rows, cols] = dot_t(u_v[rows, :], wx_v[cols, :]).astype(BF16)

    def head_spread(s, ch):
        cols = pl.ds(ch * CHW, CHW)
        rows = pl.ds(s * TOK, TOK)
        ec_v[rows, cols] = dot(csp_v[rows, :], e4_v[:, cols])
        de_v[2 * s + ch % 2] = dot(dsp_v[rows, :], e4_v[:, cols])

    t_idx = iota((BLK, GW), 0)
    s_idx = iota((BLK, GW), 1) & (BLK - 1)

    def ssd_blocks(s, ch):
        for b in range(NBLK):
            i = s * NBLK + b
            rows = pl.ds(i * BLK, BLK)
            for half in range(CHW // GW):
                off = half * GW
                cols = pl.ds(ch * CHW + off, GW)
                ce = ec_v[rows, cols]
                de = de_v[2 * s + ch % 2, b * BLK:(b + 1) * BLK, :]
                crow = jnp.sum(jnp.where(t_idx == s_idx, ce, 0.0), axis=0, keepdims=True)
                drow = jnp.sum(jnp.where(t_idx == s_idx, de, 0.0), axis=0, keepdims=True)
                decay = jnp.exp(jnp.where(t_idx >= s_idx, ce - crow, -jnp.inf))
                mix = (sc4_v[rows, :] * decay * drow).astype(BF16)
                xg = xs_v[rows, cols]
                xw = xg.astype(F32)
                xbd = jnp.concatenate([xg] * 4, axis=0) * bd_v[...]
                y_v[rows, cols] = dot(mix, xbd) + dsk_v[0:1, cols] * xw
                last = ce[BLK - 1:BLK, :]
                state = dot(bt_v[i], (xw * (jnp.exp(last - ce) * de)).astype(BF16))
                bs_v[i, ch, :, off:off + GW] = state
                ec_v[rows, cols] = jnp.exp(ce)
                el_v[i * 8:i * 8 + 8, cols] = jnp.broadcast_to(jnp.exp(last), (8, GW))
        cols = pl.ds(ch * CHW, CHW)
        end = bs_v[s * NBLK, ch]
        for b in range(1, NBLK):
            i = s * NBLK + b
            end = el_v[i * 8:i * 8 + 1, cols] * end + bs_v[i, ch]
        e_v[s, ch] = end

    def st_copy(s, ch, dst):
        return pltpu.make_async_remote_copy(src_ref=e_v.at[s, ch], dst_ref=hin_v.at[s, ch], send_sem=st_ssem.at[s, ch], recv_sem=st_rsem.at[s, ch],
                                            device_id={'seq': dst}, device_id_type=pl.DeviceIdType.MESH)

    def chain(s, ch, dst):
        cols = pl.ds(ch * CHW, CHW)
        total = el_v[(s * NBLK) * 8:(s * NBLK) * 8 + 1, cols]
        for b in range(1, NBLK):
            total = total * el_v[(s * NBLK + b) * 8:(s * NBLK + b) * 8 + 1, cols]
        e_v[s, ch] = total * hin_v[s, ch] + e_v[s, ch]
        st_copy(s, ch, dst).start()

    def first_send(s, ch):
        @pl.when(me == 0)
        def _():
            st_copy(s, ch, 1).start()

    def relay(s, *chunks):
        @pl.when(me == 1)
        def _():
            for ch in chunks:
                st_copy(s, ch, 2).wait_recv()
                chain(s, ch, 2)

    def proj_z(ch):
        cols = pl.ds(ch * CHW, CHW)
        z_v[:, cols] = dot_t(u_v[...], wz_v[cols, :]).astype(BF16)

    proj_x(0, 0, TOK)
    head_spread(0, 0)
    ssd_blocks(0, 0)

    @pl.when(me == 0)
    def _():
        pl.semaphore_wait(barrier, 3)
        st_copy(0, 0, 1).start()

    @pl.when(me != 0)
    def _():
        pl.semaphore_wait(barrier, 3)

    copies['xb'].wait()
    norm_rows(TOK, TOK)
    copies['wx1'].wait()
    load('wout', wout_h, wout_v, 6)
    load('up', up1_h, up_v, 7)
    proj_x(1)
    head_spread(0, 1)
    decay_sums(1)
    for ch in range(1, NCH):
        if ch + 1 < NCH:
            if ch >= 2:
                proj_x(ch + 1)
            else:
                proj_x(0, TOK, TOK)
            head_spread(0, ch + 1)
        else:
            block_scores(1)
            head_spread(1, 0)
        ssd_blocks(0, ch)
        first_send(0, ch)
        relay(0, ch - 1)
        if ch == 1:
            proj_x(2)
    load('down', down1_h, down_v, 8)
    load('wq', wq_h, wqkv_v.at[pl.ds(0, QH * HD), :], 9)
    load('wkv', wkv_h, wqkv_v.at[pl.ds(QH * HD, 256), :], 10)
    load('wo', wo_h, wo_v, 11)
    tab = pl.ds(pl.multiple_of(me * TOK, TOK), TOK)
    load('cos', cos_h.at[:, tab], cos_v, 12)
    load('sin', sin_h.at[:, tab], sin_v, 13)
    copies['wz'].wait()
    for ch in range(NCH):
        proj_z(ch)
        if ch + 1 < NCH:
            head_spread(1, ch + 1)
        ssd_blocks(1, ch)
        first_send(1, ch)
        if ch == 0:
            relay(0, NCH - 1)
        elif ch >= 2:
            relay(1, ch - 2)
    relay(1, NCH - 2, NCH - 1)

    def ssd_finish(s):
        for group in (range(NCH // 2), range(NCH // 2, NCH)):
            @pl.when(me == 2)
            def _(group=group):
                for ch in group:
                    st_copy(s, ch, 3).wait_recv()
                    chain(s, ch, 3)

            @pl.when(me == 3)
            def _(group=group):
                for ch in group:
                    st_copy(s, ch, 3).wait_recv()

            for ch in group:
                cols = pl.ds(ch * CHW, CHW)
                held = hin_v[s, ch]
                for b in range(NBLK):
                    i = s * NBLK + b
                    rows = pl.ds(i * BLK, BLK)
                    y_v[rows, cols] = y_v[rows, cols] + ec_v[rows, cols] * dot(c_v[rows, :], held.astype(BF16))
                    if b < NBLK - 1:
                        held = el_v[i * 8:i * 8 + 1, cols] * held + bs_v[i, ch]

        def gate(b, carry):
            rows = pl.ds(pl.multiple_of(s * TOK + b * BLK, BLK), BLK)
            ssq = jnp.zeros((BLK, 1), F32)
            for ch in range(NCH):
                yv = y_v[rows, ch * CHW:(ch + 1) * CHW]
                ssq = ssq + jnp.sum(yv * yv, axis=-1, keepdims=True)
            scale = lax.rsqrt(ssq * (1.0 / INNER) + EPS)
            for ch in range(NCH):
                cols = pl.ds(ch * CHW, CHW)
                xs_v[rows, cols] = (y_v[rows, cols] * scale * silu(z_v[rows, cols].astype(F32))).astype(BF16)
            return carry
        lax.fori_loop(0, NBLK, gate, 0, unroll=2)

        rows = pl.ds(s * TOK, TOK)
        for j in range(D // 512):
            cols = pl.ds(j * 512, 512)
            x_v[rows, cols] = (x_v[rows, cols].astype(F32) + dot(xs_v[rows, :], wout_v[:, cols])).astype(BF16)

    def mlp_up(start, count):
        rows = pl.ds(start, count)
        for j in range(FF // 256):
            gate = dot(u_v[rows, :], up_v[:, j * 256:(j + 1) * 256])
            up = dot(u_v[rows, :], up_v[:, FF + j * 256:FF + (j + 1) * 256])
            act_v[rows, j * 256:(j + 1) * 256] = (silu(gate) * up).astype(BF16)

    def mlp_down(start, count, width, out_copy=None):
        rows = pl.ds(start, count)
        for j in range(D // width):
            cols = pl.ds(j * width, width)
            x_v[rows, cols] = (x_v[rows, cols].astype(F32) + dot(act_v[rows, :], down_v[:, cols])).astype(BF16)
            if out_copy is not None:
                out_copy(j).start()

    def k_copy(s, piece, slot, dst):
        return pltpu.make_async_remote_copy(src_ref=kv_v.at[s, piece], dst_ref=kv_v.at[s, piece], send_sem=k_ssem.at[s, slot], recv_sem=k_rsem.at[s, piece],
                                            device_id={'seq': dst}, device_id_type=pl.DeviceIdType.MESH)

    def v_copy(s, piece, slot, dst):
        return pltpu.make_async_remote_copy(src_ref=vt_v.at[s, piece], dst_ref=vt_v.at[s, piece], send_sem=v_ssem.at[s, slot], recv_sem=v_rsem.at[s, piece],
                                            device_id={'seq': dst}, device_id_type=pl.DeviceIdType.MESH)

    def kv_send(s, piece, slot, dst):
        k_copy(s, piece, slot, dst).start()
        v_copy(s, piece, slot, dst).start()

    def kv_wait(s, piece):
        k_copy(s, piece, 0, 0).wait_recv()
        v_copy(s, piece, 0, 0).wait_recv()

    def kv_sent(s, piece, slot, dst):
        k_copy(s, piece, slot, dst).wait_send()
        v_copy(s, piece, slot, dst).wait_send()

    def rope(first, second):
        cos = cos_v[...]
        sin = sin_v[...]
        return first * cos - second * sin, second * cos + first * sin

    def qkv(s):
        rows = pl.ds(s * TOK, TOK)
        norm_rows(s * TOK, TOK)
        kv_t = dot_t(wqkv_v[QH * HD:, :], u_v[rows, :])
        parts = []
        for g in range(2):
            parts.extend(rope(kv_t[g * HD:g * HD + 32], kv_t[g * HD + 32:g * HD + HD]))
        kv_v[s, me] = jnp.concatenate(parts, axis=0).T.astype(BF16)
        vt_v[s, me] = kv_t[2 * HD:].astype(BF16)
        q_t = dot_t(wqkv_v[:QH * HD, :], u_v[rows, :])
        for h in range(QH):
            top = (h // 4) * HD
            lo, hi = rope(q_t[h * HD:h * HD + 32], q_t[h * HD + 32:h * HD + HD])
            qz_v[h, top:top + 32, :] = (lo * 0.125).astype(BF16)
            qz_v[h, top + 32:top + HD, :] = (hi * 0.125).astype(BF16)

        @pl.when(me == 0)
        def _():
            kv_send(s, 0, 0, 1)
            kv_send(s, 0, 1, 2)

        @pl.when(me == 1)
        def _():
            kv_send(s, 1, 0, 3)

        @pl.when(me == 2)
        def _():
            kv_send(s, 2, 0, 3)
            kv_wait(s, 0)
            kv_send(s, 0, 1, 3)

        @pl.when(me == 3)
        def _():
            kv_wait(s, 1)
            kv_send(s, 1, 0, 2)

    def attend(s, piece, first):
        causal = iota((TOK, TOK), 0) <= iota((TOK, TOK), 1)

        def score(h):
            sc_v[h % 4] = dot(kv_v[s, piece], qz_v[h])

        def soft(h):
            pieces = range(TOK // 64)

            def load_scores(r):
                sc = sc_v[h % 4, r * 64:(r + 1) * 64, :]
                return jnp.where(causal[r * 64:(r + 1) * 64], sc, -jnp.inf) if first else sc

            top = jnp.concatenate([jnp.max(load_scores(r).reshape(8, 8, TOK), axis=0) for r in pieces], axis=0)
            top = jnp.max(top, axis=0, keepdims=True)
            fix = None
            if not first:
                old = m_v[h]
                top = jnp.maximum(old, top)
                fix = jnp.exp(old - top)
            total = jnp.zeros((8, TOK), F32)
            for r in pieces:
                prob = jnp.exp(load_scores(r) - top)
                total = total + jnp.sum(prob.reshape(8, 8, TOK), axis=0)
                pr_v[h % 4, r * 64:(r + 1) * 64, :] = prob.astype(BF16)
            total = jnp.sum(total, axis=0, keepdims=True)
            l_v[h] = total if first else l_v[h] * fix + total
            m_v[h] = top
            return fix

        def mix(h, fix):
            g = h // 4
            out = dot(vt_v[s, piece, g * HD:(g + 1) * HD, :], pr_v[h % 4])
            acc_v[h] = out if first else acc_v[h] * fix + out

        score(0)
        score(1)
        fixes = {}
        for h in range(QH):
            if h + 2 < QH:
                score(h + 2)
            fixes[h] = soft(h)
            if h >= 1:
                mix(h - 1, fixes[h - 1])
        mix(QH - 1, fixes[QH - 1])

    def attention(s):
        attend(s, me, True)

        def older(piece, carry):
            early = ((me == 2) & (piece == 0)) | ((me == 3) & (piece == 1))

            @pl.when(jnp.logical_not(early))
            def _():
                kv_wait(s, piece)
            attend(s, piece, False)
            return carry
        lax.fori_loop(0, me, older, 0)
        rows = pl.ds(s * TOK, TOK)
        for pair in range(QH // 2):
            top = acc_v[2 * pair] / l_v[2 * pair]
            bot = acc_v[2 * pair + 1] / l_v[2 * pair + 1]
            att_v[:, pair * 128:(pair + 1) * 128] = jnp.concatenate([top, bot], axis=0).T.astype(BF16)
        for j in range(D // 512):
            cols = pl.ds(j * 512, 512)
            x_v[rows, cols] = (x_v[rows, cols].astype(F32) + dot(att_v[...], wo_v[:, cols])).astype(BF16)

    copies['wout'].wait()
    ssd_finish(0)
    norm_rows(0, TOK)
    copies['up'].wait()
    mlp_up(0, TOK)
    copies['down'].wait()
    mlp_down(0, TOK, 512)
    for name in ('wq', 'wkv', 'wo', 'cos', 'sin'):
        copies[name].wait()
    qkv(0)
    attention(0)
    ssd_finish(1)
    norm_rows(TOK, TOK)
    mlp_up(TOK, TOK)
    load('up', up2_h, up_v, 7)
    mlp_down(TOK, TOK, 512)
    load('down', down2_h, down_v, 8)
    qkv(1)
    attention(1)
    norm_rows(0, ROWS)
    copies['up'].wait()
    mlp_up(0, ROWS)
    copies['down'].wait()

    def out_copy(j):
        cols = pl.ds(j * 256, 256)
        return pltpu.make_async_copy(x_v.at[:, cols], out_h.at[:, cols], osem.at[j])
    mlp_down(0, ROWS, 256, out_copy)

    @pl.when(me < 3)
    def _():
        for s in range(NSEQ):
            for ch in range(NCH):
                st_copy(s, ch, 0).wait_send()
    for s in range(NSEQ):
        kv_sent(s, 0, 0, 0)

        @pl.when((me == 0) | (me == 2))
        def _():
            kv_sent(s, 0, 1, 0)
    for j in range(D // 256):
        out_copy(j).wait()


def rope_tables(seq_len):
    inv = (np.float32(ROPE_BASE) ** (-(np.arange(32, dtype=np.float32) * np.float32(2.0) / np.float32(HD)))).astype(np.float32)
    ang = (inv[:, None] * np.arange(seq_len, dtype=np.float32)[None, :]).astype(np.float32).astype(np.float64)
    return np.cos(ang).astype(np.float32), np.sin(ang).astype(np.float32)


def solution(mesh):
    n_dev = mesh.shape['seq']
    cos_t, sin_t = rope_tables(n_dev * TOK)
    any_spec = pl.BlockSpec(memory_space=pl.ANY)
    vm_spec = pl.BlockSpec(memory_space=pltpu.VMEM)
    vm = pltpu.VMEM
    call = pl.pallas_call(
        kernel,
        out_shape=jax.ShapeDtypeStruct((ROWS, D), BF16),
        in_specs=[any_spec, any_spec, vm_spec, vm_spec, vm_spec] + [any_spec] * 10,
        out_specs=any_spec,
        scratch_shapes=[
            vm((ROWS, D), BF16), vm((ROWS, D), BF16), vm((INNER, D), BF16), vm((INNER, D), BF16), vm((2 * NST, D), BF16), vm((128, D), BF16),
            vm((INNER, D), BF16), vm((D, 2 * FF), BF16), vm((FF, D), BF16), vm((QH * HD + 256, D), BF16), vm((QH * HD, D), BF16),
            vm((32, TOK), F32), vm((32, TOK), F32),
            vm((ROWS, INNER), BF16), vm((ROWS, INNER), BF16), vm((ROWS, NST), BF16), vm((ROWS, NST), BF16),
            vm((ROWS, 128), BF16), vm((ROWS, 128), BF16), vm((128, INNER), BF16), vm((GW, GW), BF16),
            vm((ROWS, INNER), F32), vm((ROWS, INNER), F32), vm((2 * NSEQ, TOK, CHW), F32), vm((NSEQ * NBLK * 8, INNER), F32), vm((8, INNER), F32),
            vm((NSEQ * NBLK, NCH, NST, CHW), F32), vm((NSEQ, NCH, NST, CHW), F32), vm((NSEQ, NCH, NST, CHW), F32), vm((ROWS, FF), BF16),
            vm((QH, 2 * HD, TOK), BF16), vm((NSEQ, 4, TOK, 128), BF16), vm((NSEQ, 4, 128, TOK), BF16),
            vm((QH, 1, TOK), F32), vm((QH, 1, TOK), F32), vm((QH, HD, TOK), F32), vm((TOK, QH * HD), BF16),
            vm((4, TOK, TOK), F32), vm((4, TOK, TOK), BF16), vm((ROWS, GW), F32), vm((NSEQ * NBLK, NST, BLK), BF16),
            pltpu.SemaphoreType.DMA((17,)), pltpu.SemaphoreType.DMA((4,)), pltpu.SemaphoreType.DMA((NSEQ, NCH)), pltpu.SemaphoreType.DMA((NSEQ, NCH)),
            pltpu.SemaphoreType.DMA((NSEQ, 2)), pltpu.SemaphoreType.DMA((NSEQ, 4)), pltpu.SemaphoreType.DMA((NSEQ, 2)), pltpu.SemaphoreType.DMA((NSEQ, 4)),
        ],
        compiler_params=pltpu.CompilerParams(collective_id=0, has_side_effects=True, vmem_limit_bytes=67_000_000),
        name='layer_stack',
    )

    def local_fn(x_loc, w_in, dt_bias, a_neg, d_skip, w_out, w_up1, w_down1, w_q, w_kv, w_o, w_up2, w_down2):
        w_q_t = w_q.transpose(1, 2, 0).reshape(QH * HD, D)
        w_kv_t = w_kv.transpose(1, 2, 3, 0).reshape(256, D)
        out = call(x_loc.reshape(ROWS, D), w_in.T, dt_bias.reshape(1, HEADS), a_neg.reshape(1, HEADS), d_skip.reshape(1, HEADS), w_out, w_up1, w_down1,
                   w_q_t, w_kv_t, w_o.reshape(QH * HD, D), w_up2, w_down2, jnp.asarray(cos_t), jnp.asarray(sin_t))
        return out.reshape(x_loc.shape)

    seq_spec = P('data', 'seq', None)
    return jax.shard_map(local_fn, mesh=mesh, in_specs=(seq_spec,) + (P(),) * 12, out_specs=seq_spec, check_vma=False)
```
